512 devices in a mesh: row: 32 (over y, x), col: 2 (over core), depth: 8 (over z).
Axes of the slice: x: 4, y: 8, z: 8, core: 2. Of those that a mesh axis runs over, the one named last changes fastest.
Arguments:
- trailing: float32 [16384, 16384], P('row', ('col', 'depth')), may hold values from -6 to 778, as said below
- panel_parts: float32 [8, 16384, 256], P('depth', 'row', 'col')
- diag_parts: float32 [8, 256, 256], P('depth'), as said below
Outputs:
- updated: float32 [16384, 16384], P('row', ('col', 'depth'))
- first_factor: float32 [16384, 256], P('row', 'col')
- second_factor: float32 [16384, 256], P('row', 'col')
The draws below stay inside these ranges and needn't reach their ends.
Inputs may be any that keep to these rules, and one draw needn't show every extreme that they name: The matrix with diagonal tile (sum of diag_parts), block column (sum of panel_parts) and trailing block A, in global order, is symmetric positive definite, and so is the trailing block after the first block column is eliminated. `diag_parts`: each layer's tile is symmetric.
All inputs are finite; a program needn't handle non-finite values.
Results may differ from the reference program's by a relative error of at most 0.000084.
Values sent between devices are 32-bit elements; how exact they have to be, the bound alone decides.
A program may use at most 128 MiB of HBM per device.

```python
import math
import jax
import jax.numpy as jnp
from jax import lax

ORDER = 16384
TILE = 256
N_ROW = 32
N_COL = 2
N_DEPTH = 8


PANEL_SCALE = 0.566


DIAG_LEAD = 64.0


def layer_weights():
    weights = jnp.linspace(1.0, 3.0, N_DEPTH, dtype=jnp.float32)
    return weights / jnp.sqrt(jnp.sum(weights * weights))


def rough_values(key, shape):
    return jnp.clip(jax.random.normal(key, shape, jnp.float32), -4.0, 4.0)


def draw_panel_parts(key, part):
    base = rough_values(jax.random.fold_in(key, 11), (N_DEPTH, ORDER, TILE))
    return base * (PANEL_SCALE * layer_weights())[:, None, None]


def draw_diag_parts(key, part):
    raw_values = rough_values(jax.random.fold_in(key, 12), (N_DEPTH, TILE, TILE))
    symmetric = (raw_values + jnp.transpose(raw_values, (0, 2, 1))) * math.sqrt(0.5)
    weights = layer_weights()
    identity = jnp.eye(TILE, dtype=jnp.float32)
    lead_share = DIAG_LEAD * weights / jnp.sum(weights)
    return symmetric * (0.5 * weights)[:, None, None] + identity[None] * lead_share[:, None, None]


def draw_trailing(key, part):
    raw_values = rough_values(jax.random.fold_in(key, 13), (ORDER, ORDER))
    symmetric = (raw_values + raw_values.T) * math.sqrt(0.5)
    shift_value = 3.0 * math.sqrt(ORDER) + 0.0075 * (math.sqrt(ORDER) + math.sqrt(TILE)) ** 2
    spread = jax.random.uniform(jax.random.fold_in(key, 14), (ORDER,), jnp.float32, 0.9, 1.1)
    full_matrix = symmetric + jnp.diag(shift_value * spread)
    per_row = ORDER // N_ROW
    per_col = ORDER // (N_COL * N_DEPTH)
    tiles_col = per_col // TILE
    slots = jnp.arange(ORDER, dtype=jnp.int32)
    row_dev = slots // per_row
    row_tile = slots % per_row // TILE
    row_global = (row_tile * N_ROW + row_dev) * TILE + slots % TILE
    group = slots // per_col
    within = slots % per_col
    tile_index = (group % N_DEPTH * tiles_col + within // TILE) * N_COL + group // N_DEPTH
    col_global = tile_index * TILE + within % TILE
    return jnp.take(jnp.take(full_matrix, row_global, axis=0), col_global, axis=1)


def setup_inputs(seed: int = 0) -> dict:
    arg_keys = jax.random.split(jax.random.key(seed), 4)
    trailing = draw_trailing(jax.random.fold_in(arg_keys[3], 71), 0)
    panel_parts = draw_panel_parts(jax.random.fold_in(arg_keys[3], 71), 0)
    diag_parts = draw_diag_parts(jax.random.fold_in(arg_keys[3], 71), 0)
    return dict(trailing=trailing, panel_parts=panel_parts, diag_parts=diag_parts)


def partner_slots():
    per_row = ORDER // N_ROW
    per_col = ORDER // (N_COL * N_DEPTH)
    tiles_col = per_col // TILE
    slots = jnp.arange(ORDER, dtype=jnp.int32)
    group = slots // per_col
    col_dev = group // N_DEPTH
    depth_dev = group % N_DEPTH
    within = slots % per_col
    tile_index = (depth_dev * tiles_col + within // TILE) * N_COL + col_dev
    global_col = tile_index * TILE + within % TILE
    global_tile = global_col // TILE
    source = global_tile % N_ROW * per_row + global_tile // N_ROW * TILE + global_col % TILE
    return source.astype(jnp.int32)

def solve_right(factor, block):
    return jax.scipy.linalg.solve_triangular(factor, block.T, lower=True).T

def reference(trailing, panel_parts, diag_parts):
    partner = partner_slots()
    diagonal = jnp.sum(diag_parts, axis=0)
    panel = jnp.sum(panel_parts, axis=0)
    lead_factor = jnp.linalg.cholesky(diagonal)
    first_factor = solve_right(lead_factor, panel)
    updated_once = trailing - jnp.dot(first_factor, jnp.take(first_factor, partner, axis=0).T, precision=lax.Precision.HIGHEST)
    next_factor = jnp.linalg.cholesky(updated_once[:TILE, :TILE])
    second_factor = solve_right(next_factor, updated_once[:, :TILE])
    keep_rows = (jnp.arange(ORDER, dtype=jnp.int32) >= TILE).astype(second_factor.dtype)
    masked = second_factor * keep_rows[:, None]
    updated = updated_once - jnp.dot(masked, jnp.take(masked, partner, axis=0).T, precision=lax.Precision.HIGHEST)
    return (updated, first_factor, second_factor)
```

```python
import functools
import jax
import jax.numpy as jnp
from jax import lax
from jax.experimental import pallas as pl
from jax.experimental.pallas import tpu as pltpu
from jax.sharding import PartitionSpec as P

f32, bf16 = jnp.float32, jnp.bfloat16
MESH = pl.DeviceIdType.MESH
NB = 32
NX, NY, NZ = 4, 8, 8
NCH = 2
ORDER_Z = (4, 3, 5, 2, 6, 1, 7)


def split2(v):
    h = v.astype(bf16)
    return h, (v - h.astype(f32)).astype(bf16)


def split3(v):
    h = v.astype(bf16)
    rest = v - h.astype(f32)
    m = rest.astype(bf16)
    return h, m, (rest - m.astype(f32)).astype(bf16)


def dot_bf(a, b, dims):
    return lax.dot_general(a, b, (dims, ((), ())), preferred_element_type=f32)


NT = ((1,), (1,))


def mul_nt(a, b):
    ah, am = a
    bh, bm = b
    return dot_bf(ah, bh, NT) + (dot_bf(ah, bm, NT) + dot_bf(am, bh, NT))


def mul_nt6(a, b):
    ah, am, al = split3(a)
    bh, bm, bl = split3(b)
    low = dot_bf(am, bm, NT) + dot_bf(ah, bl, NT) + dot_bf(al, bh, NT)
    return dot_bf(ah, bh, NT) + (dot_bf(ah, bm, NT) + dot_bf(am, bh, NT) + low)


def bc_row(v, i):
    return jnp.broadcast_to(v[i : i + 1, :], (8, 128))


def factor_block(s_ref, y_ref, first):
    groups = NB // 8
    row0 = pl.multiple_of(first, NB)
    lane0 = pl.multiple_of((first // 128) * 128, 128)
    off = first % 128
    rows = [[s_ref[pl.ds(row0 + 8 * g, 8), 128 * q : 128 * (q + 1)] for q in range(4)] for g in range(groups)]
    diag = [s_ref[pl.ds(row0 + 8 * g, 8), pl.ds(lane0, 128)] for g in range(groups)]
    sub = lax.broadcasted_iota(jnp.int32, (8, 128), 0)
    cols = []
    for j in range(NB):
        idx = jnp.full((8, 128), off + j, jnp.int32)
        cols.append(
            [
                jnp.take_along_axis(diag[g], idx, axis=1, mode="promise_in_bounds") if g >= j // 8 else None
                for g in range(groups)
            ]
        )
    scale = [jnp.ones((8, 128), f32) for _ in range(groups)]
    for j in range(NB):
        gj, rj = divmod(j, 8)
        root = lax.rsqrt(bc_row(cols[j][gj], rj))
        inv = root * root
        mult = [None] * groups
        for g in range(gj, groups):
            mult[g] = cols[j][g] * inv
        for k in range(j + 1, NB):
            gk, rk = divmod(k, 8)
            b = bc_row(cols[j][gk], rk)
            for g in range(gk, groups):
                cols[k][g] = cols[k][g] - mult[g] * b
        scale[gj] = jnp.where(sub == rj, root, scale[gj])
        if rj < 7:
            mult[gj] = jnp.where(sub > rj, mult[gj], 0.0)
        for q in range(4):
            pivot = bc_row(rows[gj][q], rj)
            for g in range(gj if rj < 7 else gj + 1, groups):
                rows[g][q] = rows[g][q] - mult[g] * pivot
    for g in range(groups):
        for q in range(4):
            y_ref[pl.ds(row0 + 8 * g, 8), 128 * q : 128 * (q + 1)] = rows[g][q] * scale[g]


def chol_inverse(s_ref, y_ref):
    i0 = lax.broadcasted_iota(jnp.int32, (256, 256), 0)
    i1 = lax.broadcasted_iota(jnp.int32, (256, 256), 1)
    s_ref[:, 256:] = jnp.where(i0 == i1, 1.0, 0.0).astype(f32)

    def body(b, carry):
        first = b * NB
        factor_block(s_ref, y_ref, first)
        h, m, l = split3(y_ref[pl.ds(pl.multiple_of(first, NB), NB), :])
        left = jnp.concatenate([h, h, m, h, m, l], axis=0)[:, :256]
        right = jnp.concatenate([h, m, h, l, m, h], axis=0)
        s_ref[...] -= dot_bf(left, right, ((0,), (0,)))
        return carry

    lax.fori_loop(0, 256 // NB, body, 0)


def comm_kernel(trail, panel, diag, d_ref, pr, cr, px, cx, pc0, rs_d, rs_p, s_rs, r_rs, s_ag, r_ag, s_c, r_c, s_x, r_x,
                s_q, r_q, s_qx, s_y, r_y, s_t, r_t):
    row, c, z = lax.axis_index("row"), lax.axis_index("col"), lax.axis_index("depth")
    x, y = lax.rem(row, NX), lax.div(row, NX)
    other = (row, 1 - c, z)
    zdev = lambda o: (row, c, lax.rem(z + o, NZ))
    xdev = lambda s: (y * NX + lax.rem(x + s + NX, NX), c, z)
    ydev = lambda s: (lax.rem(y + s + NY, NY) * NX + x, c, z)

    barrier = pltpu.get_barrier_semaphore()
    peers = [zdev(o) for o in range(1, NZ)] + [other, xdev(1), xdev(-1), ydev(1), ydev(-1)]
    for peer in peers:
        pl.semaphore_signal(barrier, inc=1, device_id=peer, device_id_type=MESH)
    pl.semaphore_wait(barrier, len(peers))

    pending = []

    def copy(src, dst, ssem, rsem, dev):
        return pltpu.make_async_remote_copy(src_ref=src, dst_ref=dst, send_sem=ssem, recv_sem=rsem, device_id=dev,
                                            device_id_type=MESH)

    def when(cond, fn):
        if cond is None:
            fn()
        else:
            pl.when(cond)(fn)

    def send(make, cond=None):
        when(cond, lambda: make().start())
        pending.append((make, cond))

    def recv(dst, ssem, rsem, cond=None):
        when(cond, lambda: copy(dst, dst, ssem, rsem, other).wait_recv())

    for o in ORDER_Z:
        send(lambda o=o: copy(diag.at[lax.rem(z + o, NZ), c], rs_d.at[o - 1], s_rs.at[0, o - 1], r_rs.at[0, o - 1], zdev(o)))
    for o in ORDER_Z:
        send(lambda o=o: copy(panel.at[lax.rem(z + o, NZ)], rs_p.at[o - 1], s_rs.at[1, o - 1], r_rs.at[1, o - 1], zdev(o)))
    source = (c == 0) & (z == 0)
    for o in ORDER_Z:
        send(lambda o=o: copy(trail.at[64 * o : 64 * (o + 1), 0:256], cr.at[o], s_c.at[o], r_c, zdev(o)), source)
    own_c = lambda: pltpu.make_async_copy(trail.at[0:64, 0:256], cr.at[0], s_c.at[0])
    when(source, lambda: own_c().start())

    total = diag[z, c]
    for o in range(1, NZ):
        recv(rs_d.at[o - 1], s_rs.at[0, o - 1], r_rs.at[0, o - 1])
        total = total + rs_d[o - 1]
    d_ref[z, c] = total
    for o in ORDER_Z:
        send(lambda o=o: copy(d_ref.at[z, c], d_ref.at[z, c], s_ag.at[0, o - 1], r_ag.at[0, o - 1], zdev(o)))

    half = pl.ds(pl.multiple_of(c * 128, 128), 128)
    total = panel[z]
    for o in range(1, NZ):
        recv(rs_p.at[o - 1], s_rs.at[1, o - 1], r_rs.at[1, o - 1])
        total = total + rs_p[o - 1]
    pr[z, :, half] = total
    for o in ORDER_Z:
        send(lambda o=o: copy(pr.at[z, :, half], pr.at[z, :, half], s_ag.at[1, o - 1], r_ag.at[1, o - 1], zdev(o)))

    when(source, lambda: own_c().wait())
    recv(cr.at[z], s_c.at[0], r_c, (c == 0) & (z != 0))
    for o in ORDER_Z:
        send(lambda o=o: copy(cr.at[z], cr.at[z], s_ag.at[2, o - 1], r_ag.at[2, o - 1], zdev(o)), c == 0)

    def from_z(o):
        return lax.rem(z + NZ - o, NZ)

    for o in range(1, NZ):
        recv(d_ref.at[from_z(o), c], s_ag.at[0, o - 1], r_ag.at[0, o - 1])
    send(lambda: copy(d_ref.at[:, c], d_ref.at[:, c], s_x.at[0], r_x.at[0], other))
    recv(d_ref.at[:, 1 - c], s_x.at[0], r_x.at[0])

    for o in range(1, NZ):
        recv(pr.at[from_z(o), :, half], s_ag.at[1, o - 1], r_ag.at[1, o - 1])
    send(lambda: copy(pr.at[:, :, half], pr.at[:, :, half], s_x.at[1], r_x.at[1], other))
    recv(pr.at[:, :, half], s_x.at[1], r_x.at[1])

    for o in range(1, NZ):
        recv(cr.at[from_z(o)], s_ag.at[2, o - 1], r_ag.at[2, o - 1], c == 0)
    send(lambda: copy(cr, cr, s_x.at[2], r_x.at[2], other), c == 0)
    recv(cr, s_x.at[2], r_x.at[2], c == 1)

    @pl.when((row == 0) & (c == 0))
    def _():
        for i in range(4):
            pc0[0, 64 * i : 64 * (i + 1), :] = pr[i]

    @pl.when((row == 0) & (c == 1))
    def _():
        for i in range(4):
            pc0[1, 64 * i : 64 * (i + 1), :] = cr[i]

    def in_set(v, values):
        ok = v == values[0]
        for w in values[1:]:
            ok = ok | (v == w)
        return ok

    rows_ch = 256 // NCH
    for ch in range(NCH):
        piece = pc0.at[c, rows_ch * ch : rows_ch * (ch + 1), :]
        recv(piece, s_q.at[0, ch], r_q.at[0, ch], (x == 0) & (y != 0))
        recv(piece, s_q.at[0, ch], r_q.at[0, ch], x != 0)
        send(lambda ch=ch, piece=piece: copy(piece, piece, s_q.at[0, ch], r_q.at[0, ch], ydev(1)),
             (x == 0) & in_set(y, (0, 1, 2, 3)))
        send(lambda ch=ch, piece=piece: copy(piece, piece, s_q.at[1, ch], r_q.at[0, ch], ydev(-1)),
             (x == 0) & in_set(y, (0, 7, 6)))
        send(lambda ch=ch, piece=piece: copy(piece, piece, s_qx.at[0, ch], r_q.at[0, ch], xdev(1)),
             (x == 0) | ((x == 1) & (c == 0)))
        send(lambda ch=ch, piece=piece: copy(piece, piece, s_qx.at[1, ch], r_q.at[0, ch], xdev(-1)),
             (x == 0) | ((x == 3) & (c == 1)))
        send(lambda ch=ch, piece=piece: copy(piece, piece, s_q.at[2, ch], r_q.at[1, ch], other))

    holder = lax.rem(x, 2) == c
    middle = lax.rem(x, 2) != c
    p = lax.rem(y - 2 * lax.rem(z, 4) + NY, NY)
    tile = lax.div(z, 4)
    xh = lax.div(x, 2)
    for buf, whole in ((px, pr), (cx, cr)):
        for j in range(2):
            @pl.when(holder & (p == j))
            def _(buf=buf, whole=whole, j=j):
                for i in range(4):
                    buf[2 * j + xh, 64 * i : 64 * (i + 1), :] = whole[4 * tile + i]

    def piece_of(a, ch, k):
        return (px, cx)[a].at[k, rows_ch * ch : rows_ch * (ch + 1), :]

    plus = (in_set(p, (0, 1, 2, 3)), in_set(p, (1, 2, 3)))
    minus = (in_set(p, (0, 7, 6)), in_set(p, (1, 0, 7, 6)))
    side = (lax.div(lax.rem(x + NX - 1, NX), 2), lax.div(lax.rem(x + 1, NX), 2))
    for a in range(2):
        for ch in range(NCH):
            for j in range(2):
                own = piece_of(a, ch, 2 * j + xh)
                recv(own, s_y.at[a, ch, j, 0], r_y.at[a, ch, j], holder & (p != j))
                send(lambda own=own, a=a, ch=ch, j=j: copy(own, own, s_y.at[a, ch, j, 0], r_y.at[a, ch, j], ydev(1)),
                     holder & plus[j])
                send(lambda own=own, a=a, ch=ch, j=j: copy(own, own, s_y.at[a, ch, j, 1], r_y.at[a, ch, j], ydev(-1)),
                     holder & minus[j])
                for s in range(2):
                    send(lambda own=own, a=a, ch=ch, j=j, s=s: copy(own, own, s_t.at[a, ch, j, s], r_t.at[a, ch, j, s],
                                                                   xdev(1 - 2 * s)), holder)
            for j in range(2):
                for s in range(2):
                    got = piece_of(a, ch, 2 * j + side[s])
                    recv(got, s_t.at[a, ch, j, s], r_t.at[a, ch, j, s], middle)
                    if j == s:
                        send(lambda got=got, a=a, ch=ch, j=j, s=s: copy(got, got, s_t.at[a, ch, j, s],
                                                                       r_t.at[a, ch, j, s], xdev(1 - 2 * s)), middle)
    for a in range(2):
        for ch in range(NCH):
            for j in range(2):
                recv(piece_of(a, ch, 2 * j + 1 - xh), s_t.at[a, ch, j, j], r_t.at[a, ch, j, j], holder)
    for ch in range(NCH):
        recv(pc0.at[1 - c, rows_ch * ch : rows_ch * (ch + 1), :], s_q.at[2, ch], r_q.at[1, ch])
    for make, cond in pending:
        when(cond, lambda make=make: make().wait_send())


def compute_kernel(trail, d_ref, pr, cr, px, cx, pc0, upd, first_out, second_out, s_ref, y_ref, a1, x1, a2, x2):
    row, c, z = lax.axis_index("row"), lax.axis_index("col"), lax.axis_index("depth")
    s_ref[:, :256] = d_ref[...]
    chol_inverse(s_ref, y_ref)
    inv1 = y_ref[:, 256:]
    lead = mul_nt6(pc0[0], inv1)
    s_ref[:, :256] = pc0[1] - mul_nt6(lead, lead)
    inv1_s = split2(inv1)
    lead_s = split2(lead)
    chol_inverse(s_ref, y_ref)
    inv2_s = split2(y_ref[:, 256:])
    half = pl.ds(pl.multiple_of(c * 128, 128), 128)

    def put(ref, rows, v):
        h, m = split2(v)
        ref[0, rows, :] = h
        ref[1, rows, :] = m

    sub = lax.broadcasted_iota(jnp.int32, (256, 256), 0)
    for t in range(2):
        rows = slice(256 * t, 256 * (t + 1))
        l1 = mul_nt(split2(pr[rows, :]), inv1_s)
        put(a1, rows, l1)
        zc = cr[rows, :] - mul_nt(split2(l1), lead_s)
        l2 = mul_nt(split2(zc), inv2_s)
        y_ref[:, :256] = l1
        y_ref[:, 256:] = l2
        first_out[rows, :] = y_ref[:, half]
        second_out[rows, :] = y_ref[:, pl.ds(pl.multiple_of(256 + c * 128, 128), 128)]
        if t == 0:
            l2 = jnp.where(row == 0, jnp.zeros_like(l2), l2)
        put(a2, rows, l2)
    for k in range(4):
        rows = slice(256 * k, 256 * (k + 1))
        l1 = mul_nt(split2(px[k]), inv1_s)
        put(x1, rows, l1)
        zc = cx[k] - mul_nt(split2(l1), lead_s)
        l2 = mul_nt(split2(zc), inv2_s)
        if k == 0:
            l2 = jnp.where((c == 0) & (z == 0), jnp.zeros_like(l2), l2)
        put(x2, rows, l2)
    for k in range(4):
        rows = slice(256 * k, 256 * (k + 1))
        for t in range(2):
            mine = slice(256 * t, 256 * (t + 1))
            one = mul_nt((a1[0, mine, :], a1[1, mine, :]), (x1[0, rows, :], x1[1, rows, :]))
            two = mul_nt((a2[0, mine, :], a2[1, mine, :]), (x2[0, rows, :], x2[1, rows, :]))
            upd[mine, rows] = trail[mine, rows] - one - two


def on_device(trailing, panel_parts, diag_parts):
    vmem = pl.BlockSpec(memory_space=pltpu.VMEM)
    dma = pltpu.SemaphoreType.DMA
    shape = lambda *s: jax.ShapeDtypeStruct(s, f32)
    d_sum, pr, cr, px, cx, pc0 = pl.pallas_call(
        comm_kernel,
        out_shape=(shape(8, 2, 16, 256), shape(8, 64, 256), shape(8, 64, 256), shape(4, 256, 256), shape(4, 256, 256),
                   shape(2, 256, 256)),
        in_specs=[pl.BlockSpec(memory_space=pl.ANY), vmem, vmem],
        out_specs=[vmem] * 6,
        scratch_shapes=[
            pltpu.VMEM((7, 16, 256), f32),
            pltpu.VMEM((7, 64, 128), f32),
            dma((2, 7)), dma((2, 7)),
            dma((3, 7)), dma((3, 7)),
            dma((8,)), dma,
            dma((3,)), dma((3,)),
            dma((3, NCH)), dma((2, NCH)), dma((2, NCH)),
            dma((2, NCH, 2, 2)), dma((2, NCH, 2)),
            dma((2, NCH, 2, 2)), dma((2, NCH, 2, 2)),
        ],
        compiler_params=pltpu.CompilerParams(collective_id=0, has_side_effects=True),
        name="move",
    )(trailing, panel_parts.reshape(8, 64, 128), diag_parts.reshape(8, 2, 16, 256))
    return pl.pallas_call(
        compute_kernel,
        out_shape=(shape(512, 1024), shape(512, 128), shape(512, 128)),
        in_specs=[vmem] * 7,
        out_specs=[vmem] * 3,
        scratch_shapes=[
            pltpu.VMEM((256, 512), f32), pltpu.VMEM((256, 512), f32),
            pltpu.VMEM((2, 512, 256), bf16), pltpu.VMEM((2, 1024, 256), bf16),
            pltpu.VMEM((2, 512, 256), bf16), pltpu.VMEM((2, 1024, 256), bf16),
        ],
        name="factor",
    )(trailing, d_sum.reshape(256, 256), pr.reshape(512, 256), cr.reshape(512, 256), px, cx, pc0)


def solution(mesh):
    return jax.shard_map(
        on_device,
        mesh=mesh,
        in_specs=(P("row", ("col", "depth")), P("depth", "row", "col"), P("depth", None, None)),
        out_specs=(P("row", ("col", "depth")), P("row", "col"), P("row", "col")),
        check_vma=False,
    )
```

```python
import functools
import jax
import jax.numpy as jnp
from jax import lax
from jax.experimental import pallas as pl
from jax.experimental.pallas import tpu as pltpu
from jax.sharding import PartitionSpec as P

f32, bf16 = jnp.float32, jnp.bfloat16
MESH = pl.DeviceIdType.MESH
NB = 32
NX, NY, NZ = 4, 8, 8
NCH = 2
ORDER_Z = (4, 3, 5, 2, 6, 1, 7)
N_SEM = 480


def split2(v):
    h = v.astype(bf16)
    return h, (v - h.astype(f32)).astype(bf16)


def split3(v):
    h = v.astype(bf16)
    rest = v - h.astype(f32)
    m = rest.astype(bf16)
    return h, m, (rest - m.astype(f32)).astype(bf16)


def dot_bf(a, b, dims):
    return lax.dot_general(a, b, (dims, ((), ())), preferred_element_type=f32)


NT = ((1,), (1,))


def mul_nt(a, b):
    ah, am = a
    bh, bm = b
    return dot_bf(ah, bh, NT) + (dot_bf(ah, bm, NT) + dot_bf(am, bh, NT))


def mul_nt6(a, b):
    ah, am, al = split3(a)
    bh, bm, bl = split3(b)
    low = dot_bf(am, bm, NT) + dot_bf(ah, bl, NT) + dot_bf(al, bh, NT)
    return dot_bf(ah, bh, NT) + (dot_bf(ah, bm, NT) + dot_bf(am, bh, NT) + low)


def bc_row(v, i):
    return jnp.broadcast_to(v[i : i + 1, :], (8, 128))


def factor_block(s_ref, y_ref, first):
    groups = NB // 8
    row0 = pl.multiple_of(first, NB)
    lane0 = pl.multiple_of((first // 128) * 128, 128)
    off = first % 128
    rows = [[s_ref[pl.ds(row0 + 8 * g, 8), 128 * q : 128 * (q + 1)] for q in range(4)] for g in range(groups)]
    diag = [s_ref[pl.ds(row0 + 8 * g, 8), pl.ds(lane0, 128)] for g in range(groups)]
    sub = lax.broadcasted_iota(jnp.int32, (8, 128), 0)
    cols = []
    for j in range(NB):
        idx = jnp.full((8, 128), off + j, jnp.int32)
        cols.append(
            [
                jnp.take_along_axis(diag[g], idx, axis=1, mode="promise_in_bounds") if g >= j // 8 else None
                for g in range(groups)
            ]
        )
    scale = [jnp.ones((8, 128), f32) for _ in range(groups)]
    for j in range(NB):
        gj, rj = divmod(j, 8)
        root = lax.rsqrt(bc_row(cols[j][gj], rj))
        inv = root * root
        mult = [None] * groups
        for g in range(gj, groups):
            mult[g] = cols[j][g] * inv
        for k in range(j + 1, NB):
            gk, rk = divmod(k, 8)
            b = bc_row(cols[j][gk], rk)
            for g in range(gk, groups):
                cols[k][g] = cols[k][g] - mult[g] * b
        scale[gj] = jnp.where(sub == rj, root, scale[gj])
        if rj < 7:
            mult[gj] = jnp.where(sub > rj, mult[gj], 0.0)
        for q in range(4):
            pivot = bc_row(rows[gj][q], rj)
            for g in range(gj if rj < 7 else gj + 1, groups):
                rows[g][q] = rows[g][q] - mult[g] * pivot
    for g in range(groups):
        for q in range(4):
            y_ref[pl.ds(row0 + 8 * g, 8), 128 * q : 128 * (q + 1)] = rows[g][q] * scale[g]


def chol_start(s_ref):
    i0 = lax.broadcasted_iota(jnp.int32, (256, 256), 0)
    i1 = lax.broadcasted_iota(jnp.int32, (256, 256), 1)
    s_ref[:, 256:] = jnp.where(i0 == i1, 1.0, 0.0).astype(f32)


def chol_steps(s_ref, y_ref, lo, hi):
    def body(b, carry):
        first = b * NB
        factor_block(s_ref, y_ref, first)
        h, m, l = split3(y_ref[pl.ds(pl.multiple_of(first, NB), NB), :])
        left = jnp.concatenate([h, h, m, h, m, l], axis=0)[:, :256]
        right = jnp.concatenate([h, m, h, l, m, h], axis=0)
        s_ref[...] -= dot_bf(left, right, ((0,), (0,)))
        return carry

    lax.fori_loop(lo, hi, body, 0)


def in_set(v, values):
    ok = v == values[0]
    for w in values[1:]:
        ok = ok | (v == w)
    return ok


def step_kernel(trail, panel, diag, upd, first_out, second_out, q, zq, part, rs_p, rr, px, cx, t_ref, s_ref, y_ref, a1, x1, a2, x2,
                sem, loc):
    row, c, z = lax.axis_index("row"), lax.axis_index("col"), lax.axis_index("depth")
    x, y = lax.rem(row, NX), lax.div(row, NX)
    other = (row, 1 - c, z)
    zdev = lambda o: (row, c, lax.rem(z + o + NZ, NZ))
    xdev = lambda s: (y * NX + lax.rem(x + s + NX, NX), c, z)
    ydev = lambda s: (lax.rem(y + s + NY, NY) * NX + x, c, z)
    half = pl.ds(pl.multiple_of(c * 128, 128), 128)
    origin = row == 0
    corner = origin & (c == 0) & (z == 0)

    get_trail = pltpu.make_async_copy(trail, t_ref, loc.at[0])
    get_trail.start()

    barrier = pltpu.get_barrier_semaphore()
    greet = lambda dev: pl.semaphore_signal(barrier, inc=1, device_id=dev, device_id_type=MESH)
    peers = [zdev(o) for o in range(1, NZ)] + [(row, 1 - c, lax.rem(z + o, NZ)) for o in range(NZ)]
    peers += [xdev(o) for o in range(1, NX)] + [ydev(o) for o in range(1, NY)]
    for peer in peers:
        greet(peer)

    @pl.when(row != 0)
    def _():
        greet((0, c, z))

    @pl.when((row != 0) & (c == 1) & (z == 0))
    def _():
        greet((0, 0, 0))

    extra = jnp.where(origin, NX * NY - 1, 0) + jnp.where(corner, NX * NY - 1, 0)
    pl.semaphore_wait(barrier, len(peers) + extra)

    counter = [0]
    pending = []

    def new(n=1):
        counter[0] += n
        assert counter[0] <= N_SEM
        return counter[0] - n

    def copy(src, dst, ssem, rsem, dev):
        return pltpu.make_async_remote_copy(src_ref=src, dst_ref=dst, send_sem=sem.at[ssem], recv_sem=sem.at[rsem],
                                            device_id=dev, device_id_type=MESH)

    def when(cond, fn):
        if cond is None:
            fn()
        else:
            pl.when(cond)(fn)

    def send_all(items, cond=None):
        makes = []
        for src, dst, rsem, dev in items:
            makes.append(functools.partial(copy, src, dst, new(), rsem, dev))

        def begin():
            for make in makes:
                make().start()

        when(cond, begin)
        for group in pending:
            if group[0] is cond:
                group[1].extend(makes)
                return
        pending.append((cond, makes))

    def send(src, dst, rsem, dev, cond=None):
        send_all([(src, dst, rsem, dev)], cond)

    def recv(dst, rsem, cond=None):
        when(cond, lambda: copy(dst, dst, rsem, rsem, other).wait_recv())

    r_z = new(21)
    for o in ORDER_Z:
        send(diag.at[row, :, half], zq.at[0, o - 1], r_z + o - 1, zdev(o))
    r_p0 = new()
    send_all([(panel.at[i], part, r_p0, (i, c, z)) for i in range(NX * NY - 1, 0, -1)], origin)
    r_c0 = new()
    halves = [(i, 128 * h, h) for i in range(NX * NY - 1, -1, -1) for h in range(2) if i or h]
    send_all([(trail.at[8 * i : 8 * i + 8, w : w + 128], q.at[2, i, :, w : w + 128], r_c0, (i, h, 0)) for i, w, h in halves],
             corner)
    own_c0 = lambda: pltpu.make_async_copy(trail.at[0:8, 0:128], q.at[2, 0, :, 0:128], loc.at[1])
    when(corner, lambda: own_c0().start())

    source = (c == 0) & (z == 0)
    xh, xp = lax.div(x, 2), lax.rem(x, 2)
    jy, qy = lax.rem(y, 2), lax.div(y, 2)
    mine = 2 * jy + xh
    r_ct = new()
    for t in range(2):
        home = (row, xp, qy + 4 * t)
        here = (xp == 0) & (qy + 4 * t == 0)
        tile_t = trail.at[256 * t : 256 * (t + 1), 0:256]
        send(tile_t, cx.at[mine], r_ct, home, source & jnp.logical_not(here))
        if t == 0:
            own_ct = lambda: pltpu.make_async_copy(trail.at[0:256, 0:256], cx.at[mine], loc.at[2])
            when(source & here, lambda: own_ct().start())
    r_rs = new(7)
    for o in ORDER_Z:
        to = lax.rem(z + o, NZ)
        send(panel.at[pl.ds(8 * to, 8)], rs_p.at[o - 1], r_rs + o - 1, zdev(o))
    r_cs = new()
    halves = [(i, 128 * h, h) for i in range(NZ - 1, -1, -1) for h in range(2) if i or h]
    send_all([(trail.at[64 * i : 64 * (i + 1), w : w + 128], rr.at[1, i, :, w : w + 128], r_cs, (row, h, i))
              for i, w, h in halves], source)
    own_cs = lambda: pltpu.make_async_copy(trail.at[0:64, 0:128], rr.at[1, 0, :, 0:128], loc.at[3])
    when(source, lambda: own_cs().start())

    r_qx, r_qy, r_qc = new(9), new(21), new(3)
    from_x = lambda o: y * NX + lax.rem(x + NX - o, NX)
    from_y = lambda o: lax.rem(y + NY - o, NY)

    def x_gather(a):
        piece = q.at[a, row, :, half]
        for o in (2, 1, 3):
            send(piece, piece, r_qx + 3 * a + o - 1, xdev(o))

    def y_gather(a):
        for o in range(1, NX):
            recv(q.at[a, from_x(o), :, half], r_qx + 3 * a + o - 1)
        piece = q.at[a, pl.ds(y * NX, NX), :, half]
        for o in (4, 3, 5, 2, 6, 1, 7):
            send(piece, piece, r_qy + 7 * a + o - 1, ydev(o))

    def core_gather(a):
        for o in range(1, NY):
            recv(q.at[a, pl.ds(from_y(o) * NX, NX), :, half], r_qy + 7 * a + o - 1)
        send(q.at[a, :, :, half], q.at[a, :, :, half], r_qc + a, other)

    def core_wait(a):
        recv(q.at[a, :, :, half], r_qc + a)

    def z_sum(a, own):
        total = own
        for o in range(1, NZ):
            recv(zq.at[a, o - 1], r_z + 7 * a + o - 1)
            total = total + zq[a, o - 1]
        q[a, row, :, half] = total

    z_sum(0, diag[row, :, half])
    x_gather(0)

    @pl.when(origin)
    def _():
        part[...] = panel[0]

    recv(part, r_p0, row != 0)
    for o in ORDER_Z:
        send(part, zq.at[1, o - 1], r_z + 7 + o - 1, zdev(o))
    when(corner, lambda: own_c0().wait())
    slice_c0 = q.at[2, row, :, half]
    recv(slice_c0, r_c0, (z == 0) & jnp.logical_not(corner))
    r_cz = new()
    send_all([(slice_c0, slice_c0, r_cz, zdev(o)) for o in ORDER_Z], z == 0)
    y_gather(0)
    z_sum(1, part[...])
    x_gather(1)
    recv(slice_c0, r_cz, z != 0)
    x_gather(2)

    holder = xp == c
    middle = xp != c
    p = lax.rem(y - 2 * lax.rem(z, 4) + NY, NY)
    rows_ch = 256 // NCH
    bufs = (px, cx)
    plus = (in_set(p, (0, 1, 2, 3)), in_set(p, (1, 2, 3)))
    minus = (in_set(p, (0, 7, 6)), in_set(p, (1, 0, 7, 6)))
    side = (lax.div(lax.rem(x + NX - 1, NX), 2), lax.div(lax.rem(x + 1, NX), 2))
    r_y = new(4 * NCH)
    r_x = new(8 * NCH)

    def at_y(a, ch, j):
        return r_y + (a * NCH + ch) * 2 + j

    def at_x(a, ch, j, s):
        return r_x + ((a * NCH + ch) * 2 + j) * 2 + s

    def piece_of(a, ch, k):
        return bufs[a].at[k, rows_ch * ch : rows_ch * (ch + 1), :]

    first = [holder & (p == j) for j in range(2)]
    later = [holder & (p != j) for j in range(2)]
    first_p = [first[j] & plus[j] for j in range(2)]
    first_m = [first[j] & minus[j] for j in range(2)]
    later_p = [later[j] & plus[j] for j in range(2)]
    later_m = [later[j] & minus[j] for j in range(2)]

    def spread_piece(a, ch, j, cond, cond_p, cond_m):
        own = piece_of(a, ch, 2 * j + xh)
        send(own, own, at_y(a, ch, j), ydev(1), cond_p)
        send(own, own, at_y(a, ch, j), ydev(-1), cond_m)
        send_all([(own, own, at_x(a, ch, j, s), xdev(1 - 2 * s)) for s in range(2)], cond)

    def tile_source(a):
        for ch in range(NCH):
            for j in range(2):
                spread_piece(a, ch, j, first[j], first_p[j], first_m[j])

    def tile_hop(a, ch):
        for j in range(2):
            recv(piece_of(a, ch, 2 * j + xh), at_y(a, ch, j), later[j])
            spread_piece(a, ch, j, later[j], later_p[j], later_m[j])
        for j in range(2):
            for s in range(2):
                got = piece_of(a, ch, 2 * j + side[s])
                recv(got, at_x(a, ch, j, s), middle)
                if j == s:
                    send(got, got, at_x(a, ch, j, s), xdev(1 - 2 * s), middle)

    def tile_last(a, ch):
        for j in range(2):
            recv(piece_of(a, ch, 2 * j + 1 - xh), at_x(a, ch, j, j), holder)

    root = holder & (jy == p)
    here = source & (xp == 0) & (qy == 0)
    when(here, lambda: own_ct().wait())
    recv(cx.at[mine], r_ct, root & jnp.logical_not(here))
    tile_source(1)

    total = panel[pl.ds(8 * z, 8)].reshape(64, 128)
    for o in range(1, NZ):
        recv(rs_p.at[o - 1], r_rs + o - 1)
        total = total + rs_p[o - 1].reshape(64, 128)
    rr[0, z, :, half] = total
    z4, zt = lax.rem(z, 4), lax.div(z, 4)
    at_home = px.at[mine, pl.ds(64 * z4, 64), half]
    is_home = (z == qy + 4 * zt) & (c == xp)
    r_pt = new(8)
    slot = r_pt + 2 * z4 + c
    send(rr.at[0, z, :, half], at_home, slot, (row, xp, qy + 4 * zt), jnp.logical_not(is_home))

    @pl.when(is_home)
    def _():
        px[mine, pl.ds(64 * z4, 64), half] = rr[0, z, :, half]

    when(source, lambda: own_cs().wait())
    recv(rr.at[1, z, :, half], r_cs, jnp.logical_not(source))
    r_rp, r_rm, r_rc = new(4), new(3), new()

    def ring_piece(i):
        return rr.at[:, lax.rem(z + i + NZ, NZ), :, half]

    send(ring_piece(0), ring_piece(0), r_rp, zdev(1))
    send(ring_piece(0), ring_piece(0), r_rm, zdev(-1))

    def ring(s):
        recv(ring_piece(-s), r_rp + s - 1)
        if s < 4:
            send(ring_piece(-s), ring_piece(-s), r_rp + s, zdev(1))
        if s < 4:
            recv(ring_piece(s), r_rm + s - 1)
        if s < 3:
            send(ring_piece(s), ring_piece(s), r_rm + s, zdev(-1))

    y_gather(1)
    y_gather(2)
    for i in range(4):
        for h in range(2):
            same = (z4 == i) & (c == h)
            recv(px.at[mine, 64 * i : 64 * (i + 1), 128 * h : 128 * (h + 1)], r_pt + 2 * i + h, root & jnp.logical_not(same))
    tile_source(0)
    core_gather(0)
    core_wait(0)

    s_ref[:, :256] = q[0].reshape(256, 256)
    chol_start(s_ref)
    chol_steps(s_ref, y_ref, 0, 4)
    tile_hop(1, 0)
    ring(1)
    chol_steps(s_ref, y_ref, 4, 8)
    tile_hop(1, 1)
    core_gather(1)
    core_gather(2)
    ring(2)
    core_wait(1)
    core_wait(2)
    inv1 = y_ref[:, 256:]
    lead = mul_nt6(q[1].reshape(256, 256), inv1)
    s_ref[:, :256] = q[2].reshape(256, 256) - mul_nt6(lead, lead)
    inv1_s = split2(inv1)
    lead_s = split2(lead)

    chol_start(s_ref)
    chol_steps(s_ref, y_ref, 0, 3)
    tile_hop(0, 0)
    ring(3)
    chol_steps(s_ref, y_ref, 3, 6)
    tile_hop(0, 1)
    ring(4)
    send(rr.at[:, :, :, half], rr.at[:, :, :, half], r_rc, other)
    chol_steps(s_ref, y_ref, 6, 8)
    inv2_s = split2(y_ref[:, 256:])
    recv(rr.at[:, :, :, half], r_rc)

    def put(ref, rows, v):
        h, m = split2(v)
        ref[0, rows, :] = h
        ref[1, rows, :] = m

    for t in range(2):
        rows = slice(256 * t, 256 * (t + 1))
        l1 = mul_nt(split2(rr[0, 4 * t : 4 * t + 4].reshape(256, 256)), inv1_s)
        put(a1, rows, l1)
        zc = rr[1, 4 * t : 4 * t + 4].reshape(256, 256) - mul_nt(split2(l1), lead_s)
        l2 = mul_nt(split2(zc), inv2_s)
        y_ref[:, :256] = l1
        y_ref[:, 256:] = l2
        first_out[rows, :] = y_ref[:, half]
        second_out[rows, :] = y_ref[:, pl.ds(pl.multiple_of(256 + c * 128, 128), 128)]
        if t == 0:
            l2 = jnp.where(row == 0, jnp.zeros_like(l2), l2)
        put(a2, rows, l2)
    for a in (1, 0):
        for ch in range(NCH):
            tile_last(a, ch)
    get_trail.wait()
    for k in range(4):
        rows = slice(256 * k, 256 * (k + 1))
        l1 = mul_nt(split2(px[k]), inv1_s)
        put(x1, rows, l1)
        zc = cx[k] - mul_nt(split2(l1), lead_s)
        l2 = mul_nt(split2(zc), inv2_s)
        if k == 0:
            l2 = jnp.where((c == 0) & (z == 0), jnp.zeros_like(l2), l2)
        put(x2, rows, l2)
        for t in range(2):
            mine_t = slice(256 * t, 256 * (t + 1))
            one = mul_nt((a1[0, mine_t, :], a1[1, mine_t, :]), (x1[0, rows, :], x1[1, rows, :]))
            two = mul_nt((a2[0, mine_t, :], a2[1, mine_t, :]), (x2[0, rows, :], x2[1, rows, :]))
            upd[mine_t, rows] = t_ref[mine_t, rows] - one - two

    def finish(makes):
        for make in makes:
            make().wait_send()

    for cond, makes in pending:
        when(cond, functools.partial(finish, makes))


def on_device(trailing, panel_parts, diag_parts):
    vmem = pl.BlockSpec(memory_space=pltpu.VMEM)
    dma = pltpu.SemaphoreType.DMA
    shape = lambda *s: jax.ShapeDtypeStruct(s, f32)
    return pl.pallas_call(
        step_kernel,
        out_shape=(shape(512, 1024), shape(512, 128), shape(512, 128)),
        in_specs=[pl.BlockSpec(memory_space=pl.ANY), vmem, vmem],
        out_specs=[vmem] * 3,
        scratch_shapes=[
            pltpu.VMEM((3, 32, 8, 256), f32), pltpu.VMEM((2, 7, 8, 128), f32), pltpu.VMEM((8, 128), f32),
            pltpu.VMEM((7, 8, 8, 128), f32), pltpu.VMEM((2, 8, 64, 256), f32),
            pltpu.VMEM((4, 256, 256), f32), pltpu.VMEM((4, 256, 256), f32), pltpu.VMEM((512, 1024), f32),
            pltpu.VMEM((256, 512), f32), pltpu.VMEM((256, 512), f32),
            pltpu.VMEM((2, 512, 256), bf16), pltpu.VMEM((2, 1024, 256), bf16),
            pltpu.VMEM((2, 512, 256), bf16), pltpu.VMEM((2, 1024, 256), bf16),
            dma((N_SEM,)), dma((4,)),
        ],
        compiler_params=pltpu.CompilerParams(collective_id=0, has_side_effects=True),
        name="step",
    )(trailing, panel_parts.reshape(64, 8, 128), diag_parts.reshape(32, 8, 256))


def solution(mesh):
    return jax.shard_map(
        on_device,
        mesh=mesh,
        in_specs=(P("row", ("col", "depth")), P("depth", "row", "col"), P("depth", None, None)),
        out_specs=(P("row", ("col", "depth")), P("row", "col"), P("row", "col")),
        check_vma=False,
    )
```

```python
import functools
import jax
import jax.numpy as jnp
from jax import lax
from jax.experimental import pallas as pl
from jax.experimental.pallas import tpu as pltpu
from jax.sharding import PartitionSpec as P

f32, bf16 = jnp.float32, jnp.bfloat16
MESH = pl.DeviceIdType.MESH
NB = 32
NX, NY, NZ = 4, 8, 8
NCH = 2
ORDER_Z = (4, 3, 5, 2, 6, 1, 7)
N_SEM = 480


def split2(v):
    h = v.astype(bf16)
    return h, (v - h.astype(f32)).astype(bf16)


def split3(v):
    h = v.astype(bf16)
    rest = v - h.astype(f32)
    m = rest.astype(bf16)
    return h, m, (rest - m.astype(f32)).astype(bf16)


def dot_bf(a, b, dims):
    return lax.dot_general(a, b, (dims, ((), ())), preferred_element_type=f32)


NT = ((1,), (1,))


def wide_left(v):
    h, m = split2(v)
    return jnp.concatenate([h, h, m], axis=1)


def wide_right(v):
    h, m = split2(v)
    return jnp.concatenate([h, m, h], axis=1)


def wide_mul(v, right):
    return dot_bf(wide_left(v), right, NT)


def mul_nt6(a, b):
    ah, am, al = split3(a)
    bh, bm, bl = split3(b)
    low = dot_bf(am, bm, NT) + dot_bf(ah, bl, NT) + dot_bf(al, bh, NT)
    return dot_bf(ah, bh, NT) + (dot_bf(ah, bm, NT) + dot_bf(am, bh, NT) + low)


def bc_row(v, i):
    return jnp.broadcast_to(v[i : i + 1, :], (8, 128))


def factor_block(s_ref, y_ref, first):
    groups = NB // 8
    row0 = pl.multiple_of(first, NB)
    lane0 = pl.multiple_of((first // 128) * 128, 128)
    off = first % 128
    rows = [[s_ref[pl.ds(row0 + 8 * g, 8), 128 * q : 128 * (q + 1)] for q in range(4)] for g in range(groups)]
    diag = [s_ref[pl.ds(row0 + 8 * g, 8), pl.ds(lane0, 128)] for g in range(groups)]
    sub = lax.broadcasted_iota(jnp.int32, (8, 128), 0)
    cols = []
    for j in range(NB):
        idx = jnp.full((8, 128), off + j, jnp.int32)
        cols.append(
            [
                jnp.take_along_axis(diag[g], idx, axis=1, mode="promise_in_bounds") if g >= j // 8 else None
                for g in range(groups)
            ]
        )
    scale = [jnp.ones((8, 128), f32) for _ in range(groups)]
    for j in range(NB):
        gj, rj = divmod(j, 8)
        root = lax.rsqrt(bc_row(cols[j][gj], rj))
        inv = root * root
        mult = [None] * groups
        for g in range(gj, groups):
            mult[g] = cols[j][g] * inv
        for k in range(j + 1, NB):
            gk, rk = divmod(k, 8)
            b = bc_row(cols[j][gk], rk)
            for g in range(gk, groups):
                cols[k][g] = cols[k][g] - mult[g] * b
        scale[gj] = jnp.where(sub == rj, root, scale[gj])
        if rj < 7:
            mult[gj] = jnp.where(sub > rj, mult[gj], 0.0)
        for q in range(4):
            pivot = bc_row(rows[gj][q], rj)
            for g in range(gj if rj < 7 else gj + 1, groups):
                rows[g][q] = rows[g][q] - mult[g] * pivot
    for g in range(groups):
        for q in range(4):
            y_ref[pl.ds(row0 + 8 * g, 8), 128 * q : 128 * (q + 1)] = rows[g][q] * scale[g]


def chol_start(s_ref):
    i0 = lax.broadcasted_iota(jnp.int32, (256, 256), 0)
    i1 = lax.broadcasted_iota(jnp.int32, (256, 256), 1)
    s_ref[:, 256:] = jnp.where(i0 == i1, 1.0, 0.0).astype(f32)


def chol_steps(s_ref, y_ref, lo, hi):
    def body(b, carry):
        first = b * NB
        factor_block(s_ref, y_ref, first)
        h, m, l = split3(y_ref[pl.ds(pl.multiple_of(first, NB), NB), :])
        left = jnp.concatenate([h, h, m, h, m, l], axis=0)[:, :256]
        right = jnp.concatenate([h, m, h, l, m, h], axis=0)
        s_ref[...] -= dot_bf(left, right, ((0,), (0,)))
        return carry

    lax.fori_loop(lo, hi, body, 0)


def in_set(v, values):
    ok = v == values[0]
    for w in values[1:]:
        ok = ok | (v == w)
    return ok


def step_kernel(trail, panel, diag, l1r, l2r, l1x, l2x, q, zq, part, rs_p, rr, px, cx, s_ref, y_ref, sem, loc):
    row, c, z = lax.axis_index("row"), lax.axis_index("col"), lax.axis_index("depth")
    x, y = lax.rem(row, NX), lax.div(row, NX)
    other = (row, 1 - c, z)
    zdev = lambda o: (row, c, lax.rem(z + o + NZ, NZ))
    xdev = lambda s: (y * NX + lax.rem(x + s + NX, NX), c, z)
    ydev = lambda s: (lax.rem(y + s + NY, NY) * NX + x, c, z)
    half = pl.ds(pl.multiple_of(c * 128, 128), 128)
    origin = row == 0
    corner = origin & (c == 0) & (z == 0)

    barrier = pltpu.get_barrier_semaphore()
    greet = lambda dev: pl.semaphore_signal(barrier, inc=1, device_id=dev, device_id_type=MESH)
    peers = [zdev(o) for o in range(1, NZ)] + [(row, 1 - c, lax.rem(z + o, NZ)) for o in range(NZ)]
    peers += [xdev(o) for o in range(1, NX)] + [ydev(o) for o in range(1, NY)]
    for peer in peers:
        greet(peer)

    @pl.when(row != 0)
    def _():
        greet((0, c, z))

    @pl.when((row != 0) & (c == 1) & (z == 0))
    def _():
        greet((0, 0, 0))

    extra = jnp.where(origin, NX * NY - 1, 0) + jnp.where(corner, NX * NY - 1, 0)
    pl.semaphore_wait(barrier, len(peers) + extra)

    counter = [0]
    pending = []

    def new(n=1):
        counter[0] += n
        assert counter[0] <= N_SEM
        return counter[0] - n

    def copy(src, dst, rsem, dev, ssem):
        return pltpu.make_async_remote_copy(src_ref=src, dst_ref=dst, send_sem=sem.at[ssem], recv_sem=sem.at[rsem],
                                            device_id=dev, device_id_type=MESH)

    def when(cond, fn):
        if cond is None:
            fn()
        else:
            pl.when(cond)(fn)

    def send_all(items, cond=None, inside=False):
        makes = []
        for item in items:
            ssem = new()
            makes.append(lambda item=item, ssem=ssem: copy(*(item() if inside else item), ssem))

        def begin():
            for make in makes:
                make().start()

        when(None if inside else cond, begin)
        for group in pending:
            if group[0] is cond:
                group[1].extend(makes)
                return
        pending.append((cond, makes))

    def send(src, dst, rsem, dev, cond=None):
        send_all([(src, dst, rsem, dev)], cond)

    def recv(dst, rsem, cond=None):
        when(cond, lambda: copy(dst, dst, rsem, other, rsem).wait_recv())

    r_z = new(21)
    for o in ORDER_Z:
        send(diag.at[row, :, half], zq.at[0, o - 1], r_z + o - 1, zdev(o))
    r_p0 = new()
    send_all([(panel.at[i], part, r_p0, (i, c, z)) for i in range(NX * NY - 1, 0, -1)], origin)
    r_c0 = new()
    halves = [(i, 128 * h, h) for i in range(NX * NY - 1, -1, -1) for h in range(2) if i or h]
    send_all([(trail.at[8 * i : 8 * i + 8, w : w + 128], q.at[2, i, :, w : w + 128], r_c0, (i, h, 0)) for i, w, h in halves],
             corner)
    own_c0 = lambda: pltpu.make_async_copy(trail.at[0:8, 0:128], q.at[2, 0, :, 0:128], loc.at[1])
    when(corner, lambda: own_c0().start())

    source = (c == 0) & (z == 0)
    xh, xp = lax.div(x, 2), lax.rem(x, 2)
    jy, qy = lax.rem(y, 2), lax.div(y, 2)
    mine = 2 * jy + xh
    r_ct = new()
    for t in range(2):
        home = (row, xp, qy + 4 * t)
        here = (xp == 0) & (qy + 4 * t == 0)
        tile_t = trail.at[256 * t : 256 * (t + 1), 0:256]
        send(tile_t, cx.at[mine], r_ct, home, source & jnp.logical_not(here))
        if t == 0:
            own_ct = lambda: pltpu.make_async_copy(trail.at[0:256, 0:256], cx.at[mine], loc.at[2])
            when(source & here, lambda: own_ct().start())
    r_rs = new(7)
    for o in ORDER_Z:
        to = lax.rem(z + o, NZ)
        send(panel.at[pl.ds(8 * to, 8)], rs_p.at[o - 1], r_rs + o - 1, zdev(o))
    r_cs = new()
    halves = [(i, 128 * h, h) for i in range(NZ - 1, -1, -1) for h in range(2) if i or h]
    send_all([(trail.at[64 * i : 64 * (i + 1), w : w + 128], rr.at[1, i, :, w : w + 128], r_cs, (row, h, i))
              for i, w, h in halves], source)
    own_cs = lambda: pltpu.make_async_copy(trail.at[0:64, 0:128], rr.at[1, 0, :, 0:128], loc.at[3])
    when(source, lambda: own_cs().start())

    r_qx, r_qy, r_qc = new(9), new(21), new(3)
    from_x = lambda o: y * NX + lax.rem(x + NX - o, NX)
    from_y = lambda o: lax.rem(y + NY - o, NY)

    def x_gather(a):
        piece = q.at[a, row, :, half]
        for o in (2, 1, 3):
            send(piece, piece, r_qx + 3 * a + o - 1, xdev(o))

    def y_gather(a):
        for o in range(1, NX):
            recv(q.at[a, from_x(o), :, half], r_qx + 3 * a + o - 1)
        piece = q.at[a, pl.ds(y * NX, NX), :, half]
        for o in (4, 3, 5, 2, 6, 1, 7):
            send(piece, piece, r_qy + 7 * a + o - 1, ydev(o))

    def core_gather(a):
        for o in range(1, NY):
            recv(q.at[a, pl.ds(from_y(o) * NX, NX), :, half], r_qy + 7 * a + o - 1)
        send(q.at[a, :, :, half], q.at[a, :, :, half], r_qc + a, other)

    def core_wait(a):
        recv(q.at[a, :, :, half], r_qc + a)

    def z_sum(a, own):
        total = own
        for o in range(1, NZ):
            recv(zq.at[a, o - 1], r_z + 7 * a + o - 1)
            total = total + zq[a, o - 1]
        q[a, row, :, half] = total

    holder = xp == c
    middle = xp != c
    p = lax.rem(y - 2 * lax.rem(z, 4) + NY, NY)
    rows_ch = 256 // NCH
    bufs = (px, cx)
    near, mid_far, far = in_set(p, (0, 1, 2, 7)), in_set(p, (3, 6)), in_set(p, (4, 5))
    away = jnp.where(in_set(p, (1, 2, 3)), 1, -1)
    side = (lax.div(lax.rem(x + NX - 1, NX), 2), lax.div(lax.rem(x + 1, NX), 2))
    r_y = new(4 * NCH)
    r_x = new(8 * NCH)
    root = holder & (jy == p)
    hold_class = [holder & near, holder & mid_far, holder & far]
    hold_near = [holder & near & (p != j) for j in range(2)]
    mid_class = [middle & near, middle & mid_far, middle & far]

    def at_y(a, ch, j):
        return r_y + (a * NCH + ch) * 2 + j

    def at_x(a, ch, j, s):
        return r_x + ((a * NCH + ch) * 2 + j) * 2 + s

    def piece_of(a, ch, k):
        return bufs[a].at[k, rows_ch * ch : rows_ch * (ch + 1), :]

    def tile_source(a):
        items = []
        for ch in range(NCH):
            own = piece_of(a, ch, mine)
            items += [(own, own, at_y(a, ch, jy), ydev(d)) for d in (1, -1)]
            items += [(own, own, at_x(a, ch, jy, s), xdev(1 - 2 * s)) for s in range(2)]
        send_all(items, root)

    def hop(a, chs, k):
        def one(ch, j, cond):
            own = lambda: piece_of(a, ch, 2 * j + xh)
            recv(own(), at_y(a, ch, j))
            items = [lambda: (own(), own(), at_y(a, ch, j), ydev(away))] if k < 2 else []
            items += [lambda s=s: (own(), own(), at_x(a, ch, j, s), xdev(1 - 2 * s)) for s in range(2)]
            send_all(items, cond, True)

        if k == 0:
            for j in range(2):

                @pl.when(hold_near[j])
                def _(j=j):
                    for ch in chs:
                        one(ch, j, hold_near[j])
        else:

            @pl.when(hold_class[k])
            def _():
                for ch in chs:
                    for j in range(2):
                        one(ch, j, hold_class[k])

    def pass_x(a, chs, k):
        @pl.when(mid_class[k])
        def _():
            for ch in chs:
                for j in range(2):
                    for s in range(2):
                        got = lambda ch=ch, j=j, s=s: piece_of(a, ch, 2 * j + side[s])
                        item = lambda ch=ch, j=j, s=s, got=got: (got(), got(), at_x(a, ch, j, s), xdev(1 - 2 * s))
                        recv(got(), at_x(a, ch, j, s))
                        if j == s:
                            send_all([item], mid_class[k], True)

    def tile_last(a):
        @pl.when(holder)
        def _():
            for ch in range(NCH):
                for j in range(2):
                    recv(piece_of(a, ch, 2 * j + 1 - xh), at_x(a, ch, j, j))

    both = tuple(range(NCH))
    z_sum(0, diag[row, :, half])
    x_gather(0)
    here = source & (xp == 0) & (qy == 0)
    when(here, lambda: own_ct().wait())
    recv(cx.at[mine], r_ct, root & jnp.logical_not(here))
    tile_source(1)

    @pl.when(origin)
    def _():
        part[...] = panel[0]

    recv(part, r_p0, row != 0)
    for o in ORDER_Z:
        send(part, zq.at[1, o - 1], r_z + 7 + o - 1, zdev(o))
    when(corner, lambda: own_c0().wait())
    slice_c0 = q.at[2, row, :, half]
    recv(slice_c0, r_c0, (z == 0) & jnp.logical_not(corner))
    r_cz = new()
    send_all([(slice_c0, slice_c0, r_cz, zdev(o)) for o in ORDER_Z], z == 0)
    y_gather(0)
    hop(1, both, 0)
    z_sum(1, part[...])
    x_gather(1)
    recv(slice_c0, r_cz, z != 0)
    x_gather(2)

    total = panel[pl.ds(8 * z, 8)].reshape(64, 128)
    for o in range(1, NZ):
        recv(rs_p.at[o - 1], r_rs + o - 1)
        total = total + rs_p[o - 1].reshape(64, 128)
    rr[0, z, :, half] = total
    z4, zt = lax.rem(z, 4), lax.div(z, 4)
    at_home = px.at[mine, pl.ds(64 * z4, 64), half]
    is_home = (z == qy + 4 * zt) & (c == xp)
    r_pt = new(8)
    slot = r_pt + 2 * z4 + c
    send(rr.at[0, z, :, half], at_home, slot, (row, xp, qy + 4 * zt), jnp.logical_not(is_home))

    @pl.when(is_home)
    def _():
        px[mine, pl.ds(64 * z4, 64), half] = rr[0, z, :, half]

    when(source, lambda: own_cs().wait())
    recv(rr.at[1, z, :, half], r_cs, jnp.logical_not(source))
    r_rp, r_rm, r_rc = new(4), new(3), new()

    def ring_piece(i):
        return rr.at[:, lax.rem(z + i + NZ, NZ), :, half]

    send(ring_piece(0), ring_piece(0), r_rp, zdev(1))
    send(ring_piece(0), ring_piece(0), r_rm, zdev(-1))

    def ring(s):
        recv(ring_piece(-s), r_rp + s - 1)
        if s < 4:
            send(ring_piece(-s), ring_piece(-s), r_rp + s, zdev(1))
            recv(ring_piece(s), r_rm + s - 1)
        if s < 3:
            send(ring_piece(s), ring_piece(s), r_rm + s, zdev(-1))

    hop(1, both, 1)
    core_gather(0)
    y_gather(1)
    y_gather(2)

    @pl.when(root)
    def _():
        for i in range(4):
            for h in range(2):
                same = (z4 == i) & (c == h)
                recv(px.at[mine, 64 * i : 64 * (i + 1), 128 * h : 128 * (h + 1)], r_pt + 2 * i + h, jnp.logical_not(same))

    tile_source(0)
    core_wait(0)

    s_ref[:, :256] = q[0].reshape(256, 256)
    chol_start(s_ref)
    pass_x(1, both, 0)
    chol_steps(s_ref, y_ref, 0, 3)
    hop(0, (0,), 0)
    hop(1, both, 2)
    ring(1)
    chol_steps(s_ref, y_ref, 3, 6)
    hop(0, both[1:], 0)
    hop(0, (0,), 1)
    pass_x(1, both, 1)
    core_gather(1)
    core_gather(2)
    ring(2)
    chol_steps(s_ref, y_ref, 6, 8)
    hop(0, both[1:], 1)
    pass_x(0, (0,), 0)
    core_wait(1)
    core_wait(2)
    inv1 = y_ref[:, 256:]
    lead = mul_nt6(q[1].reshape(256, 256), inv1)
    s_ref[:, :256] = q[2].reshape(256, 256) - mul_nt6(lead, lead)
    inv1_r = wide_right(inv1)
    lead_r = wide_right(lead)
    pass_x(1, both, 2)
    ring(3)

    chol_start(s_ref)
    chol_steps(s_ref, y_ref, 0, 2)
    hop(0, (0,), 2)
    pass_x(0, both[1:], 0)
    pass_x(0, (0,), 1)
    ring(4)
    send(rr.at[:, :, :, half], rr.at[:, :, :, half], r_rc, other)
    chol_steps(s_ref, y_ref, 2, 4)
    hop(0, both[1:], 2)
    pass_x(0, both[1:], 1)
    tile_last(1)
    chol_steps(s_ref, y_ref, 4, 6)
    pass_x(0, both, 2)
    recv(rr.at[:, :, :, half], r_rc)
    chol_steps(s_ref, y_ref, 6, 8)
    inv2_r = wide_right(y_ref[:, 256:])

    l1 = wide_mul(rr[0].reshape(512, 256), inv1_r)
    l1r[...] = l1
    l2r[...] = wide_mul(rr[1].reshape(512, 256) - wide_mul(l1, lead_r), inv2_r)
    tile_last(0)
    l1 = wide_mul(px[...].reshape(1024, 256), inv1_r)
    l1x[...] = l1
    l2x[...] = wide_mul(cx[...].reshape(1024, 256) - wide_mul(l1, lead_r), inv2_r)

    def finish(makes):
        for make in makes:
            make().wait_send()

    for cond, makes in pending:
        when(cond, functools.partial(finish, makes))


def update_kernel(trail, l1r, l2r, l1x, l2x, upd, first_out, second_out, left):
    row, c, z = lax.axis_index("row"), lax.axis_index("col"), lax.axis_index("depth")
    k = pl.program_id(0)

    @pl.when(k == 0)
    def _():
        half = pl.ds(pl.multiple_of(c * 128, 128), 128)
        first_out[...] = l1r[:, half]
        second_out[...] = l2r[:, half]
        left[:, :768] = wide_left(l1r[...])
        slot = lax.broadcasted_iota(jnp.int32, (512, 256), 0)
        left[:, 768:] = wide_left(jnp.where((slot < 256) & (row == 0), 0.0, l2r[...]))

    x2 = jnp.where((k == 0) & (c == 0) & (z == 0), 0.0, l2x[...])
    right = jnp.concatenate([wide_right(l1x[...]), wide_right(x2)], axis=1)
    upd[...] = trail[...] - dot_bf(left[...], right, NT)


def on_device(trailing, panel_parts, diag_parts):
    vmem = pl.BlockSpec(memory_space=pltpu.VMEM)
    dma = pltpu.SemaphoreType.DMA
    shape = lambda *s: jax.ShapeDtypeStruct(s, f32)
    factors = pl.pallas_call(
        step_kernel,
        out_shape=(shape(512, 256), shape(512, 256), shape(1024, 256), shape(1024, 256)),
        in_specs=[pl.BlockSpec(memory_space=pl.ANY), vmem, vmem],
        out_specs=[vmem] * 4,
        scratch_shapes=[
            pltpu.VMEM((3, 32, 8, 256), f32), pltpu.VMEM((2, 7, 8, 128), f32), pltpu.VMEM((8, 128), f32),
            pltpu.VMEM((7, 8, 8, 128), f32), pltpu.VMEM((2, 8, 64, 256), f32),
            pltpu.VMEM((4, 256, 256), f32), pltpu.VMEM((4, 256, 256), f32),
            pltpu.VMEM((256, 512), f32), pltpu.VMEM((256, 512), f32),
            dma((N_SEM,)), dma((4,)),
        ],
        compiler_params=pltpu.CompilerParams(collective_id=0, has_side_effects=True),
        name="step",
    )(trailing, panel_parts.reshape(64, 8, 128), diag_parts.reshape(32, 8, 256))
    whole = pl.BlockSpec((512, 256), lambda k: (0, 0))
    slab = pl.BlockSpec((512, 256), lambda k: (0, k))
    tile = pl.BlockSpec((256, 256), lambda k: (k, 0))
    share = pl.BlockSpec((512, 128), lambda k: (0, 0))
    return pl.pallas_call(
        update_kernel,
        grid=(4,),
        out_shape=(shape(512, 1024), shape(512, 128), shape(512, 128)),
        in_specs=[slab, whole, whole, tile, tile],
        out_specs=[slab, share, share],
        scratch_shapes=[pltpu.VMEM((512, 1536), bf16)],
        name="update",
    )(trailing, *factors)


def solution(mesh):
    return jax.shard_map(
        on_device,
        mesh=mesh,
        in_specs=(P("row", ("col", "depth")), P("depth", "row", "col"), P("depth", None, None)),
        out_specs=(P("row", ("col", "depth")), P("row", "col"), P("row", "col")),
        check_vma=False,
    )
```

```python
import functools
import jax
import jax.numpy as jnp
from jax import lax
from jax.experimental import pallas as pl
from jax.experimental.pallas import tpu as pltpu
from jax.sharding import PartitionSpec as P

f32, bf16 = jnp.float32, jnp.bfloat16
MESH = pl.DeviceIdType.MESH
NB = 32
NX, NY, NZ = 4, 8, 8
NCH = 2
ORDER_Z = (4, 3, 5, 2, 6, 1, 7)
N_SEM = 480


def split2(v):
    h = v.astype(bf16)
    return h, (v - h.astype(f32)).astype(bf16)


def split3(v):
    h = v.astype(bf16)
    rest = v - h.astype(f32)
    m = rest.astype(bf16)
    return h, m, (rest - m.astype(f32)).astype(bf16)


def dot_bf(a, b, dims):
    return lax.dot_general(a, b, (dims, ((), ())), preferred_element_type=f32)


NT = ((1,), (1,))


def wide_left(v):
    h, m = split2(v)
    return jnp.concatenate([h, h, m], axis=1)


def wide_right(v):
    h, m = split2(v)
    return jnp.concatenate([h, m, h], axis=1)


def wide_mul(v, right):
    return dot_bf(wide_left(v), right, NT)


def mul_nt6(a, b):
    ah, am, al = split3(a)
    bh, bm, bl = split3(b)
    low = dot_bf(am, bm, NT) + dot_bf(ah, bl, NT) + dot_bf(al, bh, NT)
    return dot_bf(ah, bh, NT) + (dot_bf(ah, bm, NT) + dot_bf(am, bh, NT) + low)


def bc_row(v, i):
    return jnp.broadcast_to(v[i : i + 1, :], (8, 128))


def factor_block(s_ref, y_ref, first):
    groups = NB // 8
    row0 = pl.multiple_of(first, NB)
    lane0 = pl.multiple_of((first // 128) * 128, 128)
    off = first % 128
    rows = [[s_ref[pl.ds(row0 + 8 * g, 8), 128 * q : 128 * (q + 1)] for q in range(4)] for g in range(groups)]
    diag = [s_ref[pl.ds(row0 + 8 * g, 8), pl.ds(lane0, 128)] for g in range(groups)]
    sub = lax.broadcasted_iota(jnp.int32, (8, 128), 0)
    cols = []
    for j in range(NB):
        idx = jnp.full((8, 128), off + j, jnp.int32)
        cols.append(
            [
                jnp.take_along_axis(diag[g], idx, axis=1, mode="promise_in_bounds") if g >= j // 8 else None
                for g in range(groups)
            ]
        )
    scale = [jnp.ones((8, 128), f32) for _ in range(groups)]
    for j in range(NB):
        gj, rj = divmod(j, 8)
        root = lax.rsqrt(bc_row(cols[j][gj], rj))
        inv = root * root
        mult = [None] * groups
        for g in range(gj, groups):
            mult[g] = cols[j][g] * inv
        for k in range(j + 1, NB):
            gk, rk = divmod(k, 8)
            b = bc_row(cols[j][gk], rk)
            for g in range(gk, groups):
                cols[k][g] = cols[k][g] - mult[g] * b
        scale[gj] = jnp.where(sub == rj, root, scale[gj])
        if rj < 7:
            mult[gj] = jnp.where(sub > rj, mult[gj], 0.0)
        for q in range(4):
            pivot = bc_row(rows[gj][q], rj)
            for g in range(gj if rj < 7 else gj + 1, groups):
                rows[g][q] = rows[g][q] - mult[g] * pivot
    for g in range(groups):
        for q in range(4):
            y_ref[pl.ds(row0 + 8 * g, 8), 128 * q : 128 * (q + 1)] = rows[g][q] * scale[g]


def chol_start(s_ref):
    i0 = lax.broadcasted_iota(jnp.int32, (256, 256), 0)
    i1 = lax.broadcasted_iota(jnp.int32, (256, 256), 1)
    s_ref[:, 256:] = jnp.where(i0 == i1, 1.0, 0.0).astype(f32)


def chol_steps(s_ref, y_ref, lo, hi):
    def body(b, carry):
        first = b * NB
        factor_block(s_ref, y_ref, first)
        h, m, l = split3(y_ref[pl.ds(pl.multiple_of(first, NB), NB), :])
        left = jnp.concatenate([h, h, m, h, m, l], axis=0)[:, :256]
        right = jnp.concatenate([h, m, h, l, m, h], axis=0)
        s_ref[...] -= dot_bf(left, right, ((0,), (0,)))
        return carry

    lax.fori_loop(lo, hi, body, 0)


def in_set(v, values):
    ok = v == values[0]
    for w in values[1:]:
        ok = ok | (v == w)
    return ok


def step_kernel(trail, panel, diag, l1r, l2r, l1x, l2x, q, zq, part, rs_p, rr, px, cx, s_ref, y_ref, sem, loc):
    row, c, z = lax.axis_index("row"), lax.axis_index("col"), lax.axis_index("depth")
    x, y = lax.rem(row, NX), lax.div(row, NX)
    other = (row, 1 - c, z)
    zdev = lambda o: (row, c, lax.rem(z + o + NZ, NZ))
    xdev = lambda s: (y * NX + lax.rem(x + s + NX, NX), c, z)
    ydev = lambda s: (lax.rem(y + s + NY, NY) * NX + x, c, z)
    half = pl.ds(pl.multiple_of(c * 128, 128), 128)
    origin = row == 0
    corner = origin & (c == 0) & (z == 0)

    barrier = pltpu.get_barrier_semaphore()
    greet = lambda dev: pl.semaphore_signal(barrier, inc=1, device_id=dev, device_id_type=MESH)
    peers = [zdev(o) for o in range(1, NZ)] + [(row, 1 - c, lax.rem(z + o, NZ)) for o in range(NZ)]
    peers += [xdev(o) for o in range(1, NX)] + [ydev(o) for o in range(1, NY)]
    for peer in peers:
        greet(peer)

    @pl.when(row != 0)
    def _():
        greet((0, c, z))

    @pl.when((row != 0) & (c == 1) & (z == 0))
    def _():
        greet((0, 0, 0))

    extra = jnp.where(origin, NX * NY - 1, 0) + jnp.where(corner, NX * NY - 1, 0)
    pl.semaphore_wait(barrier, len(peers) + extra)

    counter = [0]
    pending = []

    def new(n=1):
        counter[0] += n
        assert counter[0] <= N_SEM
        return counter[0] - n

    def copy(src, dst, rsem, dev, ssem):
        return pltpu.make_async_remote_copy(src_ref=src, dst_ref=dst, send_sem=sem.at[ssem], recv_sem=sem.at[rsem],
                                            device_id=dev, device_id_type=MESH)

    def when(cond, fn):
        if cond is None:
            fn()
        else:
            pl.when(cond)(fn)

    def send_all(items, cond=None, inside=False):
        makes = []
        for item in items:
            ssem = new()
            makes.append(lambda item=item, ssem=ssem: copy(*(item() if inside else item), ssem))

        def begin():
            for make in makes:
                make().start()

        when(None if inside else cond, begin)
        for group in pending:
            if group[0] is cond:
                group[1].extend(makes)
                return
        pending.append((cond, makes))

    def send(src, dst, rsem, dev, cond=None):
        send_all([(src, dst, rsem, dev)], cond)

    def recv(dst, rsem, cond=None):
        when(cond, lambda: copy(dst, dst, rsem, other, rsem).wait_recv())

    r_z = new(21)
    for o in ORDER_Z:
        send(diag.at[row, :, half], zq.at[0, o - 1], r_z + o - 1, zdev(o))
    r_p0 = new()
    send_all([(panel.at[i], part, r_p0, (i, c, z)) for i in range(NX * NY - 1, 0, -1)], origin)
    r_c0 = new()
    halves = [(i, 128 * h, h) for i in range(NX * NY - 1, -1, -1) for h in range(2) if i or h]
    send_all([(trail.at[8 * i : 8 * i + 8, w : w + 128], q.at[2, i, :, w : w + 128], r_c0, (i, h, 0)) for i, w, h in halves],
             corner)
    own_c0 = lambda: pltpu.make_async_copy(trail.at[0:8, 0:128], q.at[2, 0, :, 0:128], loc.at[1])
    when(corner, lambda: own_c0().start())

    source = (c == 0) & (z == 0)
    xh, xp = lax.div(x, 2), lax.rem(x, 2)
    jy, qy = lax.rem(y, 2), lax.div(y, 2)
    mine = 2 * jy + xh
    r_qx, r_qy, r_qc = new(9), new(21), new(3)
    from_x = lambda o: y * NX + lax.rem(x + NX - o, NX)
    from_y = lambda o: lax.rem(y + NY - o, NY)

    def x_gather(a):
        piece = q.at[a, row, :, half]
        for o in (2, 1, 3):
            send(piece, piece, r_qx + 3 * a + o - 1, xdev(o))

    def y_gather(a):
        for o in range(1, NX):
            recv(q.at[a, from_x(o), :, half], r_qx + 3 * a + o - 1)
        piece = q.at[a, pl.ds(y * NX, NX), :, half]
        for o in (4, 3, 5, 2, 6, 1, 7):
            send(piece, piece, r_qy + 7 * a + o - 1, ydev(o))

    def core_gather(a):
        for o in range(1, NY):
            recv(q.at[a, pl.ds(from_y(o) * NX, NX), :, half], r_qy + 7 * a + o - 1)
        send(q.at[a, :, :, half], q.at[a, :, :, half], r_qc + a, other)

    def core_wait(a):
        recv(q.at[a, :, :, half], r_qc + a)

    def z_sum(a, own):
        total = own
        for o in range(1, NZ):
            recv(zq.at[a, o - 1], r_z + 7 * a + o - 1)
            total = total + zq[a, o - 1]
        q[a, row, :, half] = total

    holder = xp == c
    middle = xp != c
    p = lax.rem(y - 2 * lax.rem(z, 4) + NY, NY)
    rows_ch = 256 // NCH
    bufs = (px, cx)
    near, mid_far, far = in_set(p, (0, 1, 2, 7)), in_set(p, (3, 6)), in_set(p, (4, 5))
    away = jnp.where(in_set(p, (1, 2, 3)), 1, -1)
    side = (lax.div(lax.rem(x + NX - 1, NX), 2), lax.div(lax.rem(x + 1, NX), 2))
    r_y = new(4 * NCH)
    r_x = new(8 * NCH)
    root = holder & (jy == p)
    hold_class = [holder & near, holder & mid_far, holder & far]
    hold_near = [holder & near & (p != j) for j in range(2)]
    mid_class = [middle & near, middle & mid_far, middle & far]

    def at_y(a, ch, j):
        return r_y + (a * NCH + ch) * 2 + j

    def at_x(a, ch, j, s):
        return r_x + ((a * NCH + ch) * 2 + j) * 2 + s

    def piece_of(a, ch, k):
        return bufs[a].at[k, rows_ch * ch : rows_ch * (ch + 1), :]

    def tile_source(a):
        items = []
        for ch in range(NCH):
            own = piece_of(a, ch, mine)
            items += [(own, own, at_y(a, ch, jy), ydev(d)) for d in (1, -1)]
            items += [(own, own, at_x(a, ch, jy, s), xdev(1 - 2 * s)) for s in range(2)]
        send_all(items, root)

    def hop(a, chs, k):
        def one(ch, j, cond):
            own = lambda: piece_of(a, ch, 2 * j + xh)
            recv(own(), at_y(a, ch, j))
            items = [lambda: (own(), own(), at_y(a, ch, j), ydev(away))] if k < 2 else []
            items += [lambda s=s: (own(), own(), at_x(a, ch, j, s), xdev(1 - 2 * s)) for s in range(2)]
            send_all(items, cond, True)

        if k == 0:
            for j in range(2):

                @pl.when(hold_near[j])
                def _(j=j):
                    for ch in chs:
                        one(ch, j, hold_near[j])
        else:

            @pl.when(hold_class[k])
            def _():
                for ch in chs:
                    for j in range(2):
                        one(ch, j, hold_class[k])

    def pass_x(a, chs, k):
        @pl.when(mid_class[k])
        def _():
            for ch in chs:
                for j in range(2):
                    for s in range(2):
                        got = lambda ch=ch, j=j, s=s: piece_of(a, ch, 2 * j + side[s])
                        item = lambda ch=ch, j=j, s=s, got=got: (got(), got(), at_x(a, ch, j, s), xdev(1 - 2 * s))
                        recv(got(), at_x(a, ch, j, s))
                        if j == s:
                            send_all([item], mid_class[k], True)

    def tile_last(a):
        @pl.when(holder)
        def _():
            for ch in range(NCH):
                for j in range(2):
                    recv(piece_of(a, ch, 2 * j + 1 - xh), at_x(a, ch, j, j))

    both = tuple(range(NCH))
    z_sum(0, diag[row, :, half])
    x_gather(0)

    @pl.when(origin)
    def _():
        part[...] = panel[0]

    recv(part, r_p0, row != 0)
    for o in ORDER_Z:
        send(part, zq.at[1, o - 1], r_z + 7 + o - 1, zdev(o))
    when(corner, lambda: own_c0().wait())
    slice_c0 = q.at[2, row, :, half]
    recv(slice_c0, r_c0, (z == 0) & jnp.logical_not(corner))
    r_cz = new()
    send_all([(slice_c0, slice_c0, r_cz, zdev(o)) for o in ORDER_Z], z == 0)

    r_ct = new()
    for t in range(2):
        home = (row, xp, qy + 4 * t)
        here = (xp == 0) & (qy + 4 * t == 0)
        tile_t = trail.at[256 * t : 256 * (t + 1), 0:256]
        send(tile_t, cx.at[mine], r_ct, home, source & jnp.logical_not(here))
        if t == 0:
            own_ct = lambda: pltpu.make_async_copy(trail.at[0:256, 0:256], cx.at[mine], loc.at[2])
            when(source & here, lambda: own_ct().start())
    r_rs = new(7)
    for o in ORDER_Z:
        to = lax.rem(z + o, NZ)
        send(panel.at[pl.ds(8 * to, 8)], rs_p.at[o - 1], r_rs + o - 1, zdev(o))
    r_cs = new()
    halves = [(i, 128 * h, h) for i in range(NZ - 1, -1, -1) for h in range(2) if i or h]
    send_all([(trail.at[64 * i : 64 * (i + 1), w : w + 128], rr.at[1, i, :, w : w + 128], r_cs, (row, h, i))
              for i, w, h in halves], source)
    own_cs = lambda: pltpu.make_async_copy(trail.at[0:64, 0:128], rr.at[1, 0, :, 0:128], loc.at[3])
    when(source, lambda: own_cs().start())

    y_gather(0)
    z_sum(1, part[...])
    x_gather(1)
    recv(slice_c0, r_cz, z != 0)
    x_gather(2)
    y_gather(1)
    y_gather(2)
    core_gather(0)
    z4, zt = lax.rem(z, 4), lax.div(z, 4)
    r_pt = new(8)
    r_rp, r_rm, r_rc = new(4), new(3), new()

    def ring_piece(i):
        return rr.at[:, lax.rem(z + i + NZ, NZ), :, half]

    def ring(s):
        recv(ring_piece(-s), r_rp + s - 1)
        if s < 4:
            send(ring_piece(-s), ring_piece(-s), r_rp + s, zdev(1))
            recv(ring_piece(s), r_rm + s - 1)
        if s < 3:
            send(ring_piece(s), ring_piece(s), r_rm + s, zdev(-1))

    core_wait(0)

    s_ref[:, :256] = q[0].reshape(256, 256)
    chol_start(s_ref)
    chol_steps(s_ref, y_ref, 0, 2)
    here = source & (xp == 0) & (qy == 0)
    when(here, lambda: own_ct().wait())
    recv(cx.at[mine], r_ct, root & jnp.logical_not(here))
    tile_source(1)

    total = panel[pl.ds(8 * z, 8)].reshape(64, 128)
    for o in range(1, NZ):
        recv(rs_p.at[o - 1], r_rs + o - 1)
        total = total + rs_p[o - 1].reshape(64, 128)
    rr[0, z, :, half] = total
    at_home = px.at[mine, pl.ds(64 * z4, 64), half]
    is_home = (z == qy + 4 * zt) & (c == xp)
    slot = r_pt + 2 * z4 + c
    send(rr.at[0, z, :, half], at_home, slot, (row, xp, qy + 4 * zt), jnp.logical_not(is_home))

    @pl.when(is_home)
    def _():
        px[mine, pl.ds(64 * z4, 64), half] = rr[0, z, :, half]

    when(source, lambda: own_cs().wait())
    recv(rr.at[1, z, :, half], r_cs, jnp.logical_not(source))
    send(ring_piece(0), ring_piece(0), r_rp, zdev(1))
    send(ring_piece(0), ring_piece(0), r_rm, zdev(-1))
    chol_steps(s_ref, y_ref, 2, 4)
    hop(1, both, 0)
    core_gather(1)
    core_gather(2)

    @pl.when(root)
    def _():
        for i in range(4):
            for h in range(2):
                same = (z4 == i) & (c == h)
                recv(px.at[mine, 64 * i : 64 * (i + 1), 128 * h : 128 * (h + 1)], r_pt + 2 * i + h, jnp.logical_not(same))

    tile_source(0)
    chol_steps(s_ref, y_ref, 4, 6)
    hop(1, both, 1)
    hop(0, (0,), 0)
    ring(1)
    chol_steps(s_ref, y_ref, 6, 8)
    hop(0, both[1:], 0)
    pass_x(1, both, 0)
    core_wait(1)
    core_wait(2)
    inv1 = y_ref[:, 256:]
    lead = mul_nt6(q[1].reshape(256, 256), inv1)
    s_ref[:, :256] = q[2].reshape(256, 256) - mul_nt6(lead, lead)
    inv1_r = wide_right(inv1)
    lead_r = wide_right(lead)
    hop(0, (0,), 1)
    ring(2)

    chol_start(s_ref)
    chol_steps(s_ref, y_ref, 0, 2)
    hop(0, both[1:], 1)
    hop(1, both, 2)
    pass_x(1, both, 1)
    pass_x(0, (0,), 0)
    ring(3)
    chol_steps(s_ref, y_ref, 2, 4)
    hop(0, (0,), 2)
    pass_x(0, both[1:], 0)
    pass_x(0, (0,), 1)
    ring(4)
    send(rr.at[:, :, :, half], rr.at[:, :, :, half], r_rc, other)
    chol_steps(s_ref, y_ref, 4, 6)
    hop(0, both[1:], 2)
    pass_x(1, both, 2)
    pass_x(0, both[1:], 1)
    chol_steps(s_ref, y_ref, 6, 8)
    tile_last(1)
    recv(rr.at[:, :, :, half], r_rc)
    pass_x(0, both, 2)
    inv2_r = wide_right(y_ref[:, 256:])

    l1 = wide_mul(rr[0].reshape(512, 256), inv1_r)
    l1r[...] = l1
    l2r[...] = wide_mul(rr[1].reshape(512, 256) - wide_mul(l1, lead_r), inv2_r)
    tile_last(0)
    l1 = wide_mul(px[...].reshape(1024, 256), inv1_r)
    l1x[...] = l1
    l2x[...] = wide_mul(cx[...].reshape(1024, 256) - wide_mul(l1, lead_r), inv2_r)

    def finish(makes):
        for make in makes:
            make().wait_send()

    for cond, makes in pending:
        when(cond, functools.partial(finish, makes))


def update_kernel(trail, l1r, l2r, l1x, l2x, upd, first_out, second_out, left):
    row, c, z = lax.axis_index("row"), lax.axis_index("col"), lax.axis_index("depth")
    k = pl.program_id(0)

    @pl.when(k == 0)
    def _():
        half = pl.ds(pl.multiple_of(c * 128, 128), 128)
        first_out[...] = l1r[:, half]
        second_out[...] = l2r[:, half]
        left[:, :768] = wide_left(l1r[...])
        slot = lax.broadcasted_iota(jnp.int32, (512, 256), 0)
        left[:, 768:] = wide_left(jnp.where((slot < 256) & (row == 0), 0.0, l2r[...]))

    spot = lax.broadcasted_iota(jnp.int32, (512, 256), 0)
    x2 = jnp.where((spot < 256) & (k == 0) & (c == 0) & (z == 0), 0.0, l2x[...])
    right = jnp.concatenate([wide_right(l1x[...]), wide_right(x2)], axis=1)
    upd[...] = trail[...] - dot_bf(left[...], right, NT)


def on_device(trailing, panel_parts, diag_parts):
    vmem = pl.BlockSpec(memory_space=pltpu.VMEM)
    dma = pltpu.SemaphoreType.DMA
    shape = lambda *s: jax.ShapeDtypeStruct(s, f32)
    factors = pl.pallas_call(
        step_kernel,
        out_shape=(shape(512, 256), shape(512, 256), shape(1024, 256), shape(1024, 256)),
        in_specs=[pl.BlockSpec(memory_space=pl.ANY), vmem, vmem],
        out_specs=[vmem] * 4,
        scratch_shapes=[
            pltpu.VMEM((3, 32, 8, 256), f32), pltpu.VMEM((2, 7, 8, 128), f32), pltpu.VMEM((8, 128), f32),
            pltpu.VMEM((7, 8, 8, 128), f32), pltpu.VMEM((2, 8, 64, 256), f32),
            pltpu.VMEM((4, 256, 256), f32), pltpu.VMEM((4, 256, 256), f32),
            pltpu.VMEM((256, 512), f32), pltpu.VMEM((256, 512), f32),
            dma((N_SEM,)), dma((4,)),
        ],
        compiler_params=pltpu.CompilerParams(collective_id=0, has_side_effects=True),
        name="step",
    )(trailing, panel_parts.reshape(64, 8, 128), diag_parts.reshape(32, 8, 256))
    whole = pl.BlockSpec((512, 256), lambda k: (0, 0))
    slab = pl.BlockSpec((512, 512), lambda k: (0, k))
    tile = pl.BlockSpec((512, 256), lambda k: (k, 0))
    share = pl.BlockSpec((512, 128), lambda k: (0, 0))
    return pl.pallas_call(
        update_kernel,
        grid=(2,),
        out_shape=(shape(512, 1024), shape(512, 128), shape(512, 128)),
        in_specs=[slab, whole, whole, tile, tile],
        out_specs=[slab, share, share],
        scratch_shapes=[pltpu.VMEM((512, 1536), bf16)],
        name="update",
    )(trailing, *factors)


def solution(mesh):
    return jax.shard_map(
        on_device,
        mesh=mesh,
        in_specs=(P("row", ("col", "depth")), P("depth", "row", "col"), P("depth", None, None)),
        out_specs=(P("row", ("col", "depth")), P("row", "col"), P("row", "col")),
        check_vma=False,
    )
```

```python
import functools
import jax
import jax.numpy as jnp
from jax import lax
from jax.experimental import pallas as pl
from jax.experimental.pallas import tpu as pltpu
from jax.sharding import PartitionSpec as P

f32, bf16 = jnp.float32, jnp.bfloat16
MESH = pl.DeviceIdType.MESH
NB = 32
NX, NY, NZ = 4, 8, 8
NCH = 2
ORDER_Z = (4, 3, 5, 2, 6, 1, 7)
N_SEM = 480


def split2(v):
    h = v.astype(bf16)
    return h, (v - h.astype(f32)).astype(bf16)


def split3(v):
    h = v.astype(bf16)
    rest = v - h.astype(f32)
    m = rest.astype(bf16)
    return h, m, (rest - m.astype(f32)).astype(bf16)


def dot_bf(a, b, dims):
    return lax.dot_general(a, b, (dims, ((), ())), preferred_element_type=f32)


NT = ((1,), (1,))


def wide_left(v):
    h, m = split2(v)
    return jnp.concatenate([h, h, m], axis=1)


def wide_right(v):
    h, m = split2(v)
    return jnp.concatenate([h, m, h], axis=1)


def wide_mul(v, right):
    return dot_bf(wide_left(v), right, NT)


def mul_nt6(a, b):
    ah, am, al = split3(a)
    bh, bm, bl = split3(b)
    low = dot_bf(am, bm, NT) + dot_bf(ah, bl, NT) + dot_bf(al, bh, NT)
    return dot_bf(ah, bh, NT) + (dot_bf(ah, bm, NT) + dot_bf(am, bh, NT) + low)


def bc_row(v, i):
    return jnp.broadcast_to(v[i : i + 1, :], (8, 128))


def factor_block(s_ref, y_ref, first):
    groups = NB // 8
    row0 = pl.multiple_of(first, NB)
    lane0 = pl.multiple_of((first // 128) * 128, 128)
    off = first % 128
    rows = [[s_ref[pl.ds(row0 + 8 * g, 8), 128 * q : 128 * (q + 1)] for q in range(4)] for g in range(groups)]
    diag = [s_ref[pl.ds(row0 + 8 * g, 8), pl.ds(lane0, 128)] for g in range(groups)]
    sub = lax.broadcasted_iota(jnp.int32, (8, 128), 0)
    cols = []
    for j in range(NB):
        idx = jnp.full((8, 128), off + j, jnp.int32)
        cols.append(
            [
                jnp.take_along_axis(diag[g], idx, axis=1, mode="promise_in_bounds") if g >= j // 8 else None
                for g in range(groups)
            ]
        )
    scale = [jnp.ones((8, 128), f32) for _ in range(groups)]
    for j in range(NB):
        gj, rj = divmod(j, 8)
        root = lax.rsqrt(bc_row(cols[j][gj], rj))
        inv = root * root
        mult = [None] * groups
        for g in range(gj, groups):
            mult[g] = cols[j][g] * inv
        for k in range(j + 1, NB):
            gk, rk = divmod(k, 8)
            b = bc_row(cols[j][gk], rk)
            for g in range(gk, groups):
                cols[k][g] = cols[k][g] - mult[g] * b
        scale[gj] = jnp.where(sub == rj, root, scale[gj])
        if rj < 7:
            mult[gj] = jnp.where(sub > rj, mult[gj], 0.0)
        for q in range(4):
            pivot = bc_row(rows[gj][q], rj)
            for g in range(gj if rj < 7 else gj + 1, groups):
                rows[g][q] = rows[g][q] - mult[g] * pivot
    for g in range(groups):
        for q in range(4):
            y_ref[pl.ds(row0 + 8 * g, 8), 128 * q : 128 * (q + 1)] = rows[g][q] * scale[g]


def chol_start(s_ref):
    i0 = lax.broadcasted_iota(jnp.int32, (256, 256), 0)
    i1 = lax.broadcasted_iota(jnp.int32, (256, 256), 1)
    s_ref[:, 256:] = jnp.where(i0 == i1, 1.0, 0.0).astype(f32)


def chol_steps(s_ref, y_ref, lo, hi):
    def body(b, carry):
        first = b * NB
        factor_block(s_ref, y_ref, first)
        h, m, l = split3(y_ref[pl.ds(pl.multiple_of(first, NB), NB), :])
        left = jnp.concatenate([h, h, m, h, m, l], axis=0)[:, :256]
        right = jnp.concatenate([h, m, h, l, m, h], axis=0)
        s_ref[...] -= dot_bf(left, right, ((0,), (0,)))
        return carry

    lax.fori_loop(lo, hi, body, 0)


def in_set(v, values):
    ok = v == values[0]
    for w in values[1:]:
        ok = ok | (v == w)
    return ok


def step_kernel(trail, panel, diag, l1r, l2r, l1x, l2x, q, zq, part, rs_p, rr, px, cx, s_ref, y_ref, sem, loc):
    row, c, z = lax.axis_index("row"), lax.axis_index("col"), lax.axis_index("depth")
    x, y = lax.rem(row, NX), lax.div(row, NX)
    other = (row, 1 - c, z)
    zdev = lambda o: (row, c, lax.rem(z + o + NZ, NZ))
    xdev = lambda s: (y * NX + lax.rem(x + s + NX, NX), c, z)
    ydev = lambda s: (lax.rem(y + s + NY, NY) * NX + x, c, z)
    half = pl.ds(pl.multiple_of(c * 128, 128), 128)
    origin = row == 0
    corner = origin & (c == 0) & (z == 0)

    barrier = pltpu.get_barrier_semaphore()
    greet = lambda dev: pl.semaphore_signal(barrier, inc=1, device_id=dev, device_id_type=MESH)
    peers = [zdev(o) for o in range(1, NZ)] + [(row, 1 - c, lax.rem(z + o, NZ)) for o in range(NZ)]
    peers += [xdev(o) for o in range(1, NX)] + [ydev(o) for o in range(1, NY)]
    for peer in peers:
        greet(peer)

    @pl.when(row != 0)
    def _():
        greet((0, c, z))

    @pl.when((row != 0) & (c == 1) & (z == 0))
    def _():
        greet((0, 0, 0))

    extra = jnp.where(origin, NX * NY - 1, 0) + jnp.where(corner, NX * NY - 1, 0)
    pl.semaphore_wait(barrier, len(peers) + extra)

    counter = [0]
    pending = []

    def new(n=1):
        counter[0] += n
        assert counter[0] <= N_SEM
        return counter[0] - n

    def copy(src, dst, rsem, dev, ssem):
        return pltpu.make_async_remote_copy(src_ref=src, dst_ref=dst, send_sem=sem.at[ssem], recv_sem=sem.at[rsem],
                                            device_id=dev, device_id_type=MESH)

    def when(cond, fn):
        if cond is None:
            fn()
        else:
            pl.when(cond)(fn)

    def send_all(items, cond=None, inside=False):
        makes = []
        for item in items:
            ssem = new()
            makes.append(lambda item=item, ssem=ssem: copy(*(item() if inside else item), ssem))

        def begin():
            for make in makes:
                make().start()

        when(None if inside else cond, begin)
        for group in pending:
            if group[0] is cond:
                group[1].extend(makes)
                return
        pending.append((cond, makes))

    def send(src, dst, rsem, dev, cond=None):
        send_all([(src, dst, rsem, dev)], cond)

    def recv(dst, rsem, cond=None):
        when(cond, lambda: copy(dst, dst, rsem, other, rsem).wait_recv())

    r_z = new(21)
    for o in ORDER_Z:
        send(diag.at[row, :, half], zq.at[0, o - 1], r_z + o - 1, zdev(o))
    source = (c == 0) & (z == 0)
    xh, xp = lax.div(x, 2), lax.rem(x, 2)
    jy, qy = lax.rem(y, 2), lax.div(y, 2)
    mine = 2 * jy + xh
    r_ct = new()
    for t in range(2):
        home = (row, xp, qy + 4 * t)
        here = (xp == 0) & (qy + 4 * t == 0)
        tile_t = trail.at[256 * t : 256 * (t + 1), 0:256]
        send(tile_t, cx.at[mine], r_ct, home, source & jnp.logical_not(here))
        if t == 0:
            own_ct = lambda: pltpu.make_async_copy(trail.at[0:256, 0:256], cx.at[mine], loc.at[2])
            when(source & here, lambda: own_ct().start())
    r_p0 = new()
    send_all([(panel.at[i], part, r_p0, (i, c, z)) for i in range(NX * NY - 1, 0, -1)], origin)
    r_c0 = new()
    halves = [(i, 128 * h, h) for i in range(NX * NY - 1, -1, -1) for h in range(2) if i or h]
    send_all([(trail.at[8 * i : 8 * i + 8, w : w + 128], q.at[2, i // NX, i % NX, :, w : w + 128], r_c0, (i, h, 0)) for i, w, h in halves],
             corner)
    own_c0 = lambda: pltpu.make_async_copy(trail.at[0:8, 0:128], q.at[2, 0, 0, :, 0:128], loc.at[1])
    when(corner, lambda: own_c0().start())

    r_qx, r_qy, r_qc = new(9), new(21), new(3)
    from_x = lambda o: lax.rem(x + NX - o, NX)
    from_y = lambda o: lax.rem(y + NY - o, NY)

    def y_gather(a):
        piece = q.at[a, y, x, :, half]
        for o in (4, 3, 5, 2, 6, 1, 7):
            send(piece, piece, r_qy + 7 * a + o - 1, ydev(o))

    def x_gather(a):
        for o in range(1, NY):
            recv(q.at[a, from_y(o), x, :, half], r_qy + 7 * a + o - 1)
        piece = q.at[a, :, x, :, half]
        for o in (2, 1, 3):
            send(piece, piece, r_qx + 3 * a + o - 1, xdev(o))

    def core_gather(a):
        for o in range(1, NX):
            recv(q.at[a, :, from_x(o), :, half], r_qx + 3 * a + o - 1)
        send(q.at[a, :, :, :, half], q.at[a, :, :, :, half], r_qc + a, other)

    def core_wait(a):
        recv(q.at[a, :, :, :, half], r_qc + a)

    def z_sum(a, own):
        total = own
        for o in range(1, NZ):
            recv(zq.at[a, o - 1], r_z + 7 * a + o - 1)
            total = total + zq[a, o - 1]
        q[a, y, x, :, half] = total

    holder = xp == c
    middle = xp != c
    p = lax.rem(y - 2 * lax.rem(z, 4) + NY, NY)
    rows_ch = 256 // NCH
    bufs = (px, cx)
    classes = [in_set(p, (0, 1)), in_set(p, (2, 7)), in_set(p, (3, 6)), in_set(p, (4, 5))]
    away = jnp.where(in_set(p, (1, 2, 3)), 1, -1)
    side = (lax.div(lax.rem(x + NX - 1, NX), 2), lax.div(lax.rem(x + 1, NX), 2))
    r_y = new(4 * NCH)
    r_x = new(8 * NCH)
    root = holder & (jy == p)
    hold_class = [holder & k for k in classes]
    hold_first = [holder & (p == 1 - j) for j in range(2)]
    mid_class = [middle & k for k in classes]

    def at_y(a, ch, j):
        return r_y + (a * NCH + ch) * 2 + j

    def at_x(a, ch, j, s):
        return r_x + ((a * NCH + ch) * 2 + j) * 2 + s

    def piece_of(a, ch, k):
        return bufs[a].at[k, rows_ch * ch : rows_ch * (ch + 1), :]

    def tile_source(a):
        items = []
        for ch in range(NCH):
            own = piece_of(a, ch, mine)
            items += [(own, own, at_y(a, ch, jy), ydev(d)) for d in (1, -1, jnp.where(jy == 0, 2, -2))]
            items += [(own, own, at_x(a, ch, jy, s), xdev(1 - 2 * s)) for s in range(2)]
        send_all(items, root)

    def hop(a, chs, k):
        def one(ch, j, cond):
            own = lambda: piece_of(a, ch, 2 * j + xh)
            recv(own(), at_y(a, ch, j))
            items = [lambda: (own(), own(), at_y(a, ch, j), ydev(away))] if 0 < k < 3 else []
            items += [lambda s=s: (own(), own(), at_x(a, ch, j, s), xdev(1 - 2 * s)) for s in range(2)]
            send_all(items, cond, True)

        if k == 0:
            for j in range(2):

                @pl.when(hold_first[j])
                def _(j=j):
                    for ch in chs:
                        one(ch, j, hold_first[j])
        else:

            @pl.when(hold_class[k])
            def _():
                for ch in chs:
                    for j in range(2):
                        one(ch, j, hold_class[k])

    def pass_x(a, chs, k):
        @pl.when(mid_class[k])
        def _():
            for ch in chs:
                for j in range(2):
                    for s in range(2):
                        got = lambda ch=ch, j=j, s=s: piece_of(a, ch, 2 * j + side[s])
                        item = lambda ch=ch, j=j, s=s, got=got: (got(), got(), at_x(a, ch, j, s), xdev(1 - 2 * s))
                        recv(got(), at_x(a, ch, j, s))
                        if j == s:
                            send_all([item], mid_class[k], True)

    def tile_last(a):
        @pl.when(holder)
        def _():
            for ch in range(NCH):
                for j in range(2):
                    recv(piece_of(a, ch, 2 * j + 1 - xh), at_x(a, ch, j, j))

    both = tuple(range(NCH))
    z_sum(0, diag[row, :, half])
    y_gather(0)

    @pl.when(origin)
    def _():
        part[...] = panel[0]

    recv(part, r_p0, row != 0)
    for o in ORDER_Z:
        send(part, zq.at[1, o - 1], r_z + 7 + o - 1, zdev(o))
    when(corner, lambda: own_c0().wait())
    slice_c0 = q.at[2, y, x, :, half]
    recv(slice_c0, r_c0, (z == 0) & jnp.logical_not(corner))
    r_cz = new()
    send_all([(slice_c0, slice_c0, r_cz, zdev(o)) for o in ORDER_Z], z == 0)

    r_rs = new(7)
    for o in ORDER_Z:
        to = lax.rem(z + o, NZ)
        send(panel.at[pl.ds(8 * to, 8)], rs_p.at[o - 1], r_rs + o - 1, zdev(o))
    r_cs = new()
    halves = [(i, 128 * h, h) for i in range(NZ - 1, -1, -1) for h in range(2) if i or h]
    send_all([(trail.at[64 * i : 64 * (i + 1), w : w + 128], rr.at[1, i, :, w : w + 128], r_cs, (row, h, i))
              for i, w, h in halves], source)
    own_cs = lambda: pltpu.make_async_copy(trail.at[0:64, 0:128], rr.at[1, 0, :, 0:128], loc.at[3])
    when(source, lambda: own_cs().start())

    here = source & (xp == 0) & (qy == 0)
    when(here, lambda: own_ct().wait())
    recv(cx.at[mine], r_ct, root & jnp.logical_not(here))
    tile_source(1)
    z_sum(1, part[...])
    y_gather(1)
    recv(slice_c0, r_cz, z != 0)
    y_gather(2)
    x_gather(0)
    z4, zt = lax.rem(z, 4), lax.div(z, 4)
    r_pt = new(8)
    r_rp, r_rm, r_rc = new(4), new(3), new()

    def ring_piece(i):
        return rr.at[:, lax.rem(z + i + NZ, NZ), :, half]

    def ring(s):
        recv(ring_piece(-s), r_rp + s - 1)
        if s < 4:
            send(ring_piece(-s), ring_piece(-s), r_rp + s, zdev(1))
            recv(ring_piece(s), r_rm + s - 1)
        if s < 3:
            send(ring_piece(s), ring_piece(s), r_rm + s, zdev(-1))

    core_gather(0)
    total = panel[pl.ds(8 * z, 8)].reshape(64, 128)
    for o in range(1, NZ):
        recv(rs_p.at[o - 1], r_rs + o - 1)
        total = total + rs_p[o - 1].reshape(64, 128)
    rr[0, z, :, half] = total
    at_home = px.at[mine, pl.ds(64 * z4, 64), half]
    is_home = (z == qy + 4 * zt) & (c == xp)
    slot = r_pt + 2 * z4 + c
    send(rr.at[0, z, :, half], at_home, slot, (row, xp, qy + 4 * zt), jnp.logical_not(is_home))

    @pl.when(is_home)
    def _():
        px[mine, pl.ds(64 * z4, 64), half] = rr[0, z, :, half]

    when(source, lambda: own_cs().wait())
    recv(rr.at[1, z, :, half], r_cs, jnp.logical_not(source))
    send(ring_piece(0), ring_piece(0), r_rp, zdev(1))
    send(ring_piece(0), ring_piece(0), r_rm, zdev(-1))
    hop(1, both, 0)
    x_gather(1)
    x_gather(2)
    core_wait(0)

    s_ref[:, :256] = q[0].reshape(256, 256)
    hop(1, both, 1)
    chol_start(s_ref)
    chol_steps(s_ref, y_ref, 0, 2)
    @pl.when(root)
    def _():
        for i in range(4):
            for h in range(2):
                same = (z4 == i) & (c == h)
                recv(px.at[mine, 64 * i : 64 * (i + 1), 128 * h : 128 * (h + 1)], r_pt + 2 * i + h, jnp.logical_not(same))

    tile_source(0)
    chol_steps(s_ref, y_ref, 2, 4)
    ring(1)
    core_gather(1)
    core_gather(2)
    chol_steps(s_ref, y_ref, 4, 6)
    hop(1, (0,), 2)
    pass_x(1, both, 0)
    hop(0, both, 0)
    chol_steps(s_ref, y_ref, 6, 8)
    hop(1, both[1:], 2)
    hop(0, (0,), 1)
    pass_x(1, both, 1)
    ring(2)
    core_wait(1)
    core_wait(2)
    inv1 = y_ref[:, 256:]
    lead = mul_nt6(q[1].reshape(256, 256), inv1)
    s_ref[:, :256] = q[2].reshape(256, 256) - mul_nt6(lead, lead)
    inv1_r = wide_right(inv1)
    lead_r = wide_right(lead)
    hop(0, both[1:], 1)

    chol_start(s_ref)
    chol_steps(s_ref, y_ref, 0, 2)
    hop(0, (0,), 2)
    hop(1, both, 3)
    pass_x(0, (0,), 0)
    ring(3)
    chol_steps(s_ref, y_ref, 2, 4)
    hop(0, both[1:], 2)
    pass_x(0, both[1:], 0)
    pass_x(1, both, 2)
    ring(4)
    send(rr.at[:, :, :, half], rr.at[:, :, :, half], r_rc, other)
    chol_steps(s_ref, y_ref, 4, 6)
    hop(0, (0,), 3)
    pass_x(0, both, 1)
    pass_x(1, both, 3)
    chol_steps(s_ref, y_ref, 6, 8)
    hop(0, both[1:], 3)
    pass_x(0, both, 2)
    tile_last(1)
    recv(rr.at[:, :, :, half], r_rc)
    pass_x(0, both, 3)
    inv2_r = wide_right(y_ref[:, 256:])

    l1 = wide_mul(rr[0].reshape(512, 256), inv1_r)
    l1r[...] = l1
    l2r[...] = wide_mul(rr[1].reshape(512, 256) - wide_mul(l1, lead_r), inv2_r)
    tile_last(0)
    l1 = wide_mul(px[...].reshape(1024, 256), inv1_r)
    l1x[...] = l1
    l2x[...] = wide_mul(cx[...].reshape(1024, 256) - wide_mul(l1, lead_r), inv2_r)

    def finish(makes):
        for make in makes:
            make().wait_send()

    for cond, makes in pending:
        when(cond, functools.partial(finish, makes))


def update_kernel(trail, l1r, l2r, l1x, l2x, upd, first_out, second_out, left):
    row, c, z = lax.axis_index("row"), lax.axis_index("col"), lax.axis_index("depth")
    k = pl.program_id(0)

    @pl.when(k == 0)
    def _():
        half = pl.ds(pl.multiple_of(c * 128, 128), 128)
        first_out[...] = l1r[:, half]
        second_out[...] = l2r[:, half]
        left[:, :768] = wide_left(l1r[...])
        slot = lax.broadcasted_iota(jnp.int32, (512, 256), 0)
        left[:, 768:] = wide_left(jnp.where((slot < 256) & (row == 0), 0.0, l2r[...]))

    spot = lax.broadcasted_iota(jnp.int32, (512, 256), 0)
    x2 = jnp.where((spot < 256) & (k == 0) & (c == 0) & (z == 0), 0.0, l2x[...])
    right = jnp.concatenate([wide_right(l1x[...]), wide_right(x2)], axis=1)
    upd[...] = trail[...] - dot_bf(left[...], right, NT)


def on_device(trailing, panel_parts, diag_parts):
    vmem = pl.BlockSpec(memory_space=pltpu.VMEM)
    dma = pltpu.SemaphoreType.DMA
    shape = lambda *s: jax.ShapeDtypeStruct(s, f32)
    factors = pl.pallas_call(
        step_kernel,
        out_shape=(shape(512, 256), shape(512, 256), shape(1024, 256), shape(1024, 256)),
        in_specs=[pl.BlockSpec(memory_space=pl.ANY), vmem, vmem],
        out_specs=[vmem] * 4,
        scratch_shapes=[
            pltpu.VMEM((3, NY, NX, 8, 256), f32), pltpu.VMEM((2, 7, 8, 128), f32), pltpu.VMEM((8, 128), f32),
            pltpu.VMEM((7, 8, 8, 128), f32), pltpu.VMEM((2, 8, 64, 256), f32),
            pltpu.VMEM((4, 256, 256), f32), pltpu.VMEM((4, 256, 256), f32),
            pltpu.VMEM((256, 512), f32), pltpu.VMEM((256, 512), f32),
            dma((N_SEM,)), dma((4,)),
        ],
        compiler_params=pltpu.CompilerParams(collective_id=0, has_side_effects=True),
        name="step",
    )(trailing, panel_parts.reshape(64, 8, 128), diag_parts.reshape(32, 8, 256))
    whole = pl.BlockSpec((512, 256), lambda k: (0, 0))
    slab = pl.BlockSpec((512, 512), lambda k: (0, k))
    tile = pl.BlockSpec((512, 256), lambda k: (k, 0))
    share = pl.BlockSpec((512, 128), lambda k: (0, 0))
    return pl.pallas_call(
        update_kernel,
        grid=(2,),
        out_shape=(shape(512, 1024), shape(512, 128), shape(512, 128)),
        in_specs=[slab, whole, whole, tile, tile],
        out_specs=[slab, share, share],
        scratch_shapes=[pltpu.VMEM((512, 1536), bf16)],
        name="update",
    )(trailing, *factors)


def solution(mesh):
    return jax.shard_map(
        on_device,
        mesh=mesh,
        in_specs=(P("row", ("col", "depth")), P("depth", "row", "col"), P("depth", None, None)),
        out_specs=(P("row", ("col", "depth")), P("row", "col"), P("row", "col")),
        check_vma=False,
    )
```

```python
import functools
import jax
import jax.numpy as jnp
from jax import lax
from jax.experimental import pallas as pl
from jax.experimental.pallas import tpu as pltpu
from jax.sharding import PartitionSpec as P

f32, bf16 = jnp.float32, jnp.bfloat16
MESH = pl.DeviceIdType.MESH
NB = 32
NX, NY, NZ = 4, 8, 8
NCH = 2
ORDER_Z = (4, 3, 5, 2, 6, 1, 7)
N_SEM = 480


def split2(v):
    h = v.astype(bf16)
    return h, (v - h.astype(f32)).astype(bf16)


def split3(v):
    h = v.astype(bf16)
    rest = v - h.astype(f32)
    m = rest.astype(bf16)
    return h, m, (rest - m.astype(f32)).astype(bf16)


def dot_bf(a, b, dims):
    return lax.dot_general(a, b, (dims, ((), ())), preferred_element_type=f32)


NT = ((1,), (1,))


def wide_left(v):
    h, m = split2(v)
    return jnp.concatenate([h, h, m], axis=1)


def wide_right(v):
    h, m = split2(v)
    return jnp.concatenate([h, m, h], axis=1)


def wide_mul(v, right):
    return dot_bf(wide_left(v), right, NT)


def mul_nt6(a, b):
    ah, am, al = split3(a)
    bh, bm, bl = split3(b)
    low = dot_bf(am, bm, NT) + dot_bf(ah, bl, NT) + dot_bf(al, bh, NT)
    return dot_bf(ah, bh, NT) + (dot_bf(ah, bm, NT) + dot_bf(am, bh, NT) + low)


def bc_row(v, i):
    return jnp.broadcast_to(v[i : i + 1, :], (8, 128))


def factor_block(s_ref, y_ref, first):
    groups = NB // 8
    row0 = pl.multiple_of(first, NB)
    lane0 = pl.multiple_of((first // 128) * 128, 128)
    off = first % 128
    rows = [[s_ref[pl.ds(row0 + 8 * g, 8), 128 * q : 128 * (q + 1)] for q in range(4)] for g in range(groups)]
    diag = [s_ref[pl.ds(row0 + 8 * g, 8), pl.ds(lane0, 128)] for g in range(groups)]
    sub = lax.broadcasted_iota(jnp.int32, (8, 128), 0)
    cols = []
    for j in range(NB):
        idx = jnp.full((8, 128), off + j, jnp.int32)
        cols.append(
            [
                jnp.take_along_axis(diag[g], idx, axis=1, mode="promise_in_bounds") if g >= j // 8 else None
                for g in range(groups)
            ]
        )
    scale = [jnp.ones((8, 128), f32) for _ in range(groups)]
    for j in range(NB):
        gj, rj = divmod(j, 8)
        root = lax.rsqrt(bc_row(cols[j][gj], rj))
        inv = root * root
        mult = [None] * groups
        for g in range(gj, groups):
            mult[g] = cols[j][g] * inv
        for k in range(j + 1, NB):
            gk, rk = divmod(k, 8)
            b = bc_row(cols[j][gk], rk)
            for g in range(gk, groups):
                cols[k][g] = cols[k][g] - mult[g] * b
        scale[gj] = jnp.where(sub == rj, root, scale[gj])
        if rj < 7:
            mult[gj] = jnp.where(sub > rj, mult[gj], 0.0)
        for q in range(4):
            pivot = bc_row(rows[gj][q], rj)
            for g in range(gj if rj < 7 else gj + 1, groups):
                rows[g][q] = rows[g][q] - mult[g] * pivot
    for g in range(groups):
        for q in range(4):
            y_ref[pl.ds(row0 + 8 * g, 8), 128 * q : 128 * (q + 1)] = rows[g][q] * scale[g]


def chol_start(s_ref):
    i0 = lax.broadcasted_iota(jnp.int32, (256, 256), 0)
    i1 = lax.broadcasted_iota(jnp.int32, (256, 256), 1)
    s_ref[:, 256:] = jnp.where(i0 == i1, 1.0, 0.0).astype(f32)


def chol_steps(s_ref, y_ref, lo, hi):
    def body(b, carry):
        first = b * NB
        factor_block(s_ref, y_ref, first)
        h, m, l = split3(y_ref[pl.ds(pl.multiple_of(first, NB), NB), :])
        left = jnp.concatenate([h, h, m, h, m, l], axis=0)[:, :256]
        right = jnp.concatenate([h, m, h, l, m, h], axis=0)
        s_ref[...] -= dot_bf(left, right, ((0,), (0,)))
        return carry

    lax.fori_loop(lo, hi, body, 0)


def in_set(v, values):
    ok = v == values[0]
    for w in values[1:]:
        ok = ok | (v == w)
    return ok


def step_kernel(trail, panel, diag, l1r, l2r, l1x, l2x, q, zq, part, rs_p, rr, px, cx, s_ref, y_ref, sem, loc):
    row, c, z = lax.axis_index("row"), lax.axis_index("col"), lax.axis_index("depth")
    x, y = lax.rem(row, NX), lax.div(row, NX)
    other = (row, 1 - c, z)
    zdev = lambda o: (row, c, lax.rem(z + o + NZ, NZ))
    xdev = lambda s: (y * NX + lax.rem(x + s + NX, NX), c, z)
    ydev = lambda s: (lax.rem(y + s + NY, NY) * NX + x, c, z)
    half = pl.ds(pl.multiple_of(c * 128, 128), 128)
    origin = row == 0
    corner = origin & (c == 0) & (z == 0)

    barrier = pltpu.get_barrier_semaphore()
    greet = lambda dev: pl.semaphore_signal(barrier, inc=1, device_id=dev, device_id_type=MESH)
    peers = [zdev(o) for o in range(1, NZ)] + [(row, 1 - c, lax.rem(z + o, NZ)) for o in range(NZ)]
    peers += [xdev(o) for o in range(1, NX)] + [ydev(o) for o in range(1, NY)]
    for peer in peers:
        greet(peer)

    @pl.when(row != 0)
    def _():
        greet((0, c, z))

    @pl.when((row != 0) & (c == 1) & (z == 0))
    def _():
        greet((0, 0, 0))

    extra = jnp.where(origin, NX * NY - 1, 0) + jnp.where(corner, NX * NY - 1, 0)
    pl.semaphore_wait(barrier, len(peers) + extra)

    counter = [0]
    pending = []

    def new(n=1):
        counter[0] += n
        assert counter[0] <= N_SEM
        return counter[0] - n

    def copy(src, dst, rsem, dev, ssem):
        return pltpu.make_async_remote_copy(src_ref=src, dst_ref=dst, send_sem=sem.at[ssem], recv_sem=sem.at[rsem],
                                            device_id=dev, device_id_type=MESH)

    def when(cond, fn):
        if cond is None:
            fn()
        else:
            pl.when(cond)(fn)

    def send_all(items, cond=None, inside=False):
        makes = []
        for item in items:
            ssem = new()
            makes.append(lambda item=item, ssem=ssem: copy(*(item() if inside else item), ssem))

        def begin():
            for make in makes:
                make().start()

        when(None if inside else cond, begin)
        for group in pending:
            if group[0] is cond:
                group[1].extend(makes)
                return
        pending.append((cond, makes))

    def send(src, dst, rsem, dev, cond=None):
        send_all([(src, dst, rsem, dev)], cond)

    def recv(dst, rsem, cond=None):
        when(cond, lambda: copy(dst, dst, rsem, other, rsem).wait_recv())

    r_z = new(21)
    for o in ORDER_Z:
        send(diag.at[row, :, half], zq.at[0, o - 1], r_z + o - 1, zdev(o))
    source = (c == 0) & (z == 0)
    xh, xp = lax.div(x, 2), lax.rem(x, 2)
    jy, qy = lax.rem(y, 2), lax.div(y, 2)
    mine = 2 * jy + xh
    r_ct = new()
    for t in range(2):
        home = (row, xp, qy + 4 * t)
        here = (xp == 0) & (qy + 4 * t == 0)
        tile_t = trail.at[256 * t : 256 * (t + 1), 0:256]
        send(tile_t, cx.at[mine], r_ct, home, source & jnp.logical_not(here))
        if t == 0:
            own_ct = lambda: pltpu.make_async_copy(trail.at[0:256, 0:256], cx.at[mine], loc.at[2])
            when(source & here, lambda: own_ct().start())
    r_p0 = new()
    send_all([(panel.at[i], part, r_p0, (i, c, z)) for i in range(NX * NY - 1, 0, -1)], origin)
    r_c0 = new()
    halves = [(i, 128 * h, h) for i in range(NX * NY - 1, -1, -1) for h in range(2) if i or h]
    send_all([(trail.at[8 * i : 8 * i + 8, w : w + 128], q.at[2, i // NX, i % NX, :, w : w + 128], r_c0, (i, h, 0)) for i, w, h in halves],
             corner)
    own_c0 = lambda: pltpu.make_async_copy(trail.at[0:8, 0:128], q.at[2, 0, 0, :, 0:128], loc.at[1])
    when(corner, lambda: own_c0().start())

    r_qx, r_qy, r_qc = new(9), new(21), new(3)
    from_x = lambda o: lax.rem(x + NX - o, NX)
    from_y = lambda o: lax.rem(y + NY - o, NY)

    def y_gather(a):
        piece = q.at[a, y, x, :, half]
        for o in (4, 3, 5, 2, 6, 1, 7):
            send(piece, piece, r_qy + 7 * a + o - 1, ydev(o))

    def x_gather(a):
        for o in range(1, NY):
            recv(q.at[a, from_y(o), x, :, half], r_qy + 7 * a + o - 1)
        piece = q.at[a, :, x, :, half]
        for o in (2, 1, 3):
            send(piece, piece, r_qx + 3 * a + o - 1, xdev(o))

    def core_gather(a):
        for o in range(1, NX):
            recv(q.at[a, :, from_x(o), :, half], r_qx + 3 * a + o - 1)
        send(q.at[a, :, :, :, half], q.at[a, :, :, :, half], r_qc + a, other)

    def core_wait(a):
        recv(q.at[a, :, :, :, half], r_qc + a)

    def z_sum(a, own):
        total = own
        for o in range(1, NZ):
            recv(zq.at[a, o - 1], r_z + 7 * a + o - 1)
            total = total + zq[a, o - 1]
        q[a, y, x, :, half] = total

    holder = xp == c
    middle = xp != c
    p = lax.rem(y - 2 * lax.rem(z, 4) + NY, NY)
    rows_ch = 256 // NCH
    bufs = (px, cx)
    classes = [in_set(p, (0, 1)), in_set(p, (2, 7)), in_set(p, (3, 6)), in_set(p, (4, 5))]
    away = jnp.where(in_set(p, (1, 2, 3)), 1, -1)
    side = (lax.div(lax.rem(x + NX - 1, NX), 2), lax.div(lax.rem(x + 1, NX), 2))
    r_y = new(4 * NCH)
    r_x = new(8 * NCH)
    root = holder & (jy == p)
    hold_class = [holder & k for k in classes]
    hold_first = [holder & (p == 1 - j) for j in range(2)]
    mid_class = [middle & k for k in classes]

    def at_y(a, ch, j):
        return r_y + (a * NCH + ch) * 2 + j

    def at_x(a, ch, j, s):
        return r_x + ((a * NCH + ch) * 2 + j) * 2 + s

    def piece_of(a, ch, k):
        return bufs[a].at[k, rows_ch * ch : rows_ch * (ch + 1), :]

    def tile_source(a):
        items = []
        for ch in range(NCH):
            own = piece_of(a, ch, mine)
            items += [(own, own, at_y(a, ch, jy), ydev(d)) for d in (1, -1, jnp.where(jy == 0, 2, -2))]
            items += [(own, own, at_x(a, ch, jy, s), xdev(1 - 2 * s)) for s in range(2)]
        send_all(items, root)

    def hop(a, chs, k):
        def one(ch, j, cond):
            own = lambda: piece_of(a, ch, 2 * j + xh)
            recv(own(), at_y(a, ch, j))
            items = [lambda: (own(), own(), at_y(a, ch, j), ydev(away))] if 0 < k < 3 else []
            items += [lambda s=s: (own(), own(), at_x(a, ch, j, s), xdev(1 - 2 * s)) for s in range(2)]
            send_all(items, cond, True)

        if k == 0:
            for j in range(2):

                @pl.when(hold_first[j])
                def _(j=j):
                    for ch in chs:
                        one(ch, j, hold_first[j])
        else:

            @pl.when(hold_class[k])
            def _():
                for ch in chs:
                    for j in range(2):
                        one(ch, j, hold_class[k])

    def pass_x(a, chs, k):
        @pl.when(mid_class[k])
        def _():
            for ch in chs:
                for j in range(2):
                    for s in range(2):
                        got = lambda ch=ch, j=j, s=s: piece_of(a, ch, 2 * j + side[s])
                        item = lambda ch=ch, j=j, s=s, got=got: (got(), got(), at_x(a, ch, j, s), xdev(1 - 2 * s))
                        recv(got(), at_x(a, ch, j, s))
                        if j == s:
                            send_all([item], mid_class[k], True)

    def tile_last(a):
        @pl.when(holder)
        def _():
            for ch in range(NCH):
                for j in range(2):
                    recv(piece_of(a, ch, 2 * j + 1 - xh), at_x(a, ch, j, j))

    both = tuple(range(NCH))
    z_sum(0, diag[row, :, half])
    y_gather(0)

    @pl.when(origin)
    def _():
        part[...] = panel[0]

    recv(part, r_p0, row != 0)
    for o in ORDER_Z:
        send(part, zq.at[1, o - 1], r_z + 7 + o - 1, zdev(o))
    when(corner, lambda: own_c0().wait())
    slice_c0 = q.at[2, y, x, :, half]
    recv(slice_c0, r_c0, (z == 0) & jnp.logical_not(corner))
    r_cz = new()
    send_all([(slice_c0, slice_c0, r_cz, zdev(o)) for o in ORDER_Z], z == 0)

    r_rs = new(7)
    for o in ORDER_Z:
        to = lax.rem(z + o, NZ)
        send(panel.at[pl.ds(8 * to, 8)], rs_p.at[o - 1], r_rs + o - 1, zdev(o))
    r_cs = new()
    halves = [(i, 128 * h, h) for i in range(NZ - 1, -1, -1) for h in range(2) if i or h]
    send_all([(trail.at[64 * i : 64 * (i + 1), w : w + 128], rr.at[1, i, :, w : w + 128], r_cs, (row, h, i))
              for i, w, h in halves], source)
    own_cs = lambda: pltpu.make_async_copy(trail.at[0:64, 0:128], rr.at[1, 0, :, 0:128], loc.at[3])
    when(source, lambda: own_cs().start())

    here = source & (xp == 0) & (qy == 0)
    when(here, lambda: own_ct().wait())
    recv(cx.at[mine], r_ct, root & jnp.logical_not(here))
    tile_source(1)
    z_sum(1, part[...])
    y_gather(1)
    recv(slice_c0, r_cz, z != 0)
    y_gather(2)
    x_gather(0)
    z4, zt = lax.rem(z, 4), lax.div(z, 4)
    r_pt = new(8)
    r_rp, r_rm, r_rc = new(4), new(3), new()

    def ring_piece(i):
        return rr.at[:, lax.rem(z + i + NZ, NZ), :, half]

    def ring(s):
        recv(ring_piece(-s), r_rp + s - 1)
        if s < 4:
            send(ring_piece(-s), ring_piece(-s), r_rp + s, zdev(1))
            recv(ring_piece(s), r_rm + s - 1)
        if s < 3:
            send(ring_piece(s), ring_piece(s), r_rm + s, zdev(-1))

    core_gather(0)
    total = panel[pl.ds(8 * z, 8)].reshape(64, 128)
    for o in range(1, NZ):
        recv(rs_p.at[o - 1], r_rs + o - 1)
        total = total + rs_p[o - 1].reshape(64, 128)
    rr[0, z, :, half] = total
    at_home = px.at[mine, pl.ds(64 * z4, 64), half]
    is_home = (z == qy + 4 * zt) & (c == xp)
    slot = r_pt + 2 * z4 + c
    send(rr.at[0, z, :, half], at_home, slot, (row, xp, qy + 4 * zt), jnp.logical_not(is_home))

    @pl.when(is_home)
    def _():
        px[mine, pl.ds(64 * z4, 64), half] = rr[0, z, :, half]

    when(source, lambda: own_cs().wait())
    recv(rr.at[1, z, :, half], r_cs, jnp.logical_not(source))
    send(ring_piece(0), ring_piece(0), r_rp, zdev(1))
    send(ring_piece(0), ring_piece(0), r_rm, zdev(-1))
    hop(1, both, 0)
    x_gather(1)
    hop(1, both, 1)
    x_gather(2)
    core_wait(0)

    s_ref[:, :256] = q[0].reshape(256, 256)
    chol_start(s_ref)
    chol_steps(s_ref, y_ref, 0, 2)
    @pl.when(root)
    def _():
        for i in range(4):
            for h in range(2):
                same = (z4 == i) & (c == h)
                recv(px.at[mine, 64 * i : 64 * (i + 1), 128 * h : 128 * (h + 1)], r_pt + 2 * i + h, jnp.logical_not(same))

    tile_source(0)
    chol_steps(s_ref, y_ref, 2, 4)
    hop(1, (0,), 2)
    ring(1)
    core_gather(1)
    core_gather(2)
    chol_steps(s_ref, y_ref, 4, 6)
    hop(1, both[1:], 2)
    pass_x(1, both, 0)
    hop(0, both, 0)
    chol_steps(s_ref, y_ref, 6, 8)
    hop(0, (0,), 1)
    hop(1, (0,), 3)
    pass_x(1, both, 1)
    ring(2)
    core_wait(1)
    core_wait(2)
    inv1 = y_ref[:, 256:]
    lead = mul_nt6(q[1].reshape(256, 256), inv1)
    s_ref[:, :256] = q[2].reshape(256, 256) - mul_nt6(lead, lead)
    inv1_r = wide_right(inv1)
    lead_r = wide_right(lead)
    hop(0, both[1:], 1)

    chol_start(s_ref)
    chol_steps(s_ref, y_ref, 0, 2)
    hop(0, (0,), 2)
    hop(1, both[1:], 3)
    pass_x(0, (0,), 0)
    ring(3)
    chol_steps(s_ref, y_ref, 2, 4)
    hop(0, both[1:], 2)
    pass_x(0, both[1:], 0)
    pass_x(1, both, 2)
    pass_x(1, (0,), 3)
    ring(4)
    send(rr.at[:, :, :, half], rr.at[:, :, :, half], r_rc, other)
    chol_steps(s_ref, y_ref, 4, 6)
    hop(0, (0,), 3)
    pass_x(0, both, 1)
    pass_x(1, both[1:], 3)
    chol_steps(s_ref, y_ref, 6, 8)
    hop(0, both[1:], 3)
    pass_x(0, both, 2)
    recv(rr.at[:, :, :, half], r_rc)
    inv2_r = wide_right(y_ref[:, 256:])

    l1 = wide_mul(rr[0].reshape(512, 256), inv1_r)
    l1r[...] = l1
    l2r[...] = wide_mul(rr[1].reshape(512, 256) - wide_mul(l1, lead_r), inv2_r)
    pass_x(0, both, 3)
    tile_last(1)
    tile_last(0)
    l1 = wide_mul(px[...].reshape(1024, 256), inv1_r)
    l1x[...] = l1
    l2x[...] = wide_mul(cx[...].reshape(1024, 256) - wide_mul(l1, lead_r), inv2_r)

    def finish(makes):
        for make in makes:
            make().wait_send()

    for cond, makes in pending:
        when(cond, functools.partial(finish, makes))


def update_kernel(trail, l1r, l2r, l1x, l2x, upd, first_out, second_out, left):
    row, c, z = lax.axis_index("row"), lax.axis_index("col"), lax.axis_index("depth")
    k = pl.program_id(0)

    @pl.when(k == 0)
    def _():
        half = pl.ds(pl.multiple_of(c * 128, 128), 128)
        first_out[...] = l1r[:, half]
        second_out[...] = l2r[:, half]
        left[:, :768] = wide_left(l1r[...])
        slot = lax.broadcasted_iota(jnp.int32, (512, 256), 0)
        left[:, 768:] = wide_left(jnp.where((slot < 256) & (row == 0), 0.0, l2r[...]))

    spot = lax.broadcasted_iota(jnp.int32, (512, 256), 0)
    x2 = jnp.where((spot < 256) & (k == 0) & (c == 0) & (z == 0), 0.0, l2x[...])
    right = jnp.concatenate([wide_right(l1x[...]), wide_right(x2)], axis=1)
    upd[...] = trail[...] - dot_bf(left[...], right, NT)


def on_device(trailing, panel_parts, diag_parts):
    vmem = pl.BlockSpec(memory_space=pltpu.VMEM)
    dma = pltpu.SemaphoreType.DMA
    shape = lambda *s: jax.ShapeDtypeStruct(s, f32)
    factors = pl.pallas_call(
        step_kernel,
        out_shape=(shape(512, 256), shape(512, 256), shape(1024, 256), shape(1024, 256)),
        in_specs=[pl.BlockSpec(memory_space=pl.ANY), vmem, vmem],
        out_specs=[vmem] * 4,
        scratch_shapes=[
            pltpu.VMEM((3, NY, NX, 8, 256), f32), pltpu.VMEM((2, 7, 8, 128), f32), pltpu.VMEM((8, 128), f32),
            pltpu.VMEM((7, 8, 8, 128), f32), pltpu.VMEM((2, 8, 64, 256), f32),
            pltpu.VMEM((4, 256, 256), f32), pltpu.VMEM((4, 256, 256), f32),
            pltpu.VMEM((256, 512), f32), pltpu.VMEM((256, 512), f32),
            dma((N_SEM,)), dma((4,)),
        ],
        compiler_params=pltpu.CompilerParams(collective_id=0, has_side_effects=True),
        name="step",
    )(trailing, panel_parts.reshape(64, 8, 128), diag_parts.reshape(32, 8, 256))
    whole = pl.BlockSpec((512, 256), lambda k: (0, 0))
    slab = pl.BlockSpec((512, 512), lambda k: (0, k))
    tile = pl.BlockSpec((512, 256), lambda k: (k, 0))
    share = pl.BlockSpec((512, 128), lambda k: (0, 0))
    return pl.pallas_call(
        update_kernel,
        grid=(2,),
        out_shape=(shape(512, 1024), shape(512, 128), shape(512, 128)),
        in_specs=[slab, whole, whole, tile, tile],
        out_specs=[slab, share, share],
        scratch_shapes=[pltpu.VMEM((512, 1536), bf16)],
        name="update",
    )(trailing, *factors)


def solution(mesh):
    return jax.shard_map(
        on_device,
        mesh=mesh,
        in_specs=(P("row", ("col", "depth")), P("depth", "row", "col"), P("depth", None, None)),
        out_specs=(P("row", ("col", "depth")), P("row", "col"), P("row", "col")),
        check_vma=False,
    )
```
